512 devices in a mesh: chan: 64 (over z, y_hi, core), wall: 8 (over x, y_lo).
Axes of the slice: x: 4, y: 8 (y_hi: 4, y_lo: 2; y = y_hi * 2 + y_lo), z: 8, core: 2. Of those that a mesh axis runs over, the one named last changes fastest.
Arguments:
- coords: float32 [3, 64, 8, 4096], P(None, 'chan', 'wall'), as said below
- masses: float32 [64, 8, 4096], P('chan', 'wall'), may hold values from 0.5 to 2
- counts: int32 [64, 8, 16], P('chan', 'wall'), may hold values from 64 to 256
- lists: int32 [64, 8, 5, 16, 2], P('chan', 'wall'), may hold values from 0 to 47, as said below
Outputs:
- density: float32 [64, 8, 4096], P('chan', 'wall')
The draws below stay inside these ranges and needn't reach their ends.
Inputs may be any that keep to these rules, and one draw needn't show every extreme that they name: `lists`: each row of 2 entries names different tiles; tile t of extended slab s is s * 16 + t, slab 0 the lower cross-wall neighbour, 1 the slab itself, 2 the upper neighbour. `coords`: channel components lie in [0, 1), cross-wall and depth components in [0, 8).
All inputs are finite; a program needn't handle non-finite values.
Results may differ from the reference program's by a relative error of at most 0.0003.
Values sent between devices are 32-bit elements; how exact they have to be, the bound alone decides.
A program may use at most 64 MiB of HBM per device.

```python
import math
import jax
import jax.numpy as jnp
from jax import lax

TILE = 256
TILE_DEV = 16
NB = 2
R = 4
CHAN_SLABS = 64
WALL_SLABS = 8
PART = 4096


def draw_coords(key, part):
    unit = jax.random.uniform(key, (3, CHAN_SLABS, WALL_SLABS, TILE_DEV * TILE), jnp.float32)
    extent = jnp.array([1.0, 2.0 * R, 2.0 * R], jnp.float32).reshape(3, 1, 1, 1)
    return (unit * extent * 0.9999).astype(jnp.float32)


def draw_lists(key, part):
    choices_count = 3 * TILE_DEV
    scores = jax.random.randint(key, (CHAN_SLABS, WALL_SLABS, R + 1, TILE_DEV, choices_count), 0, 1 << 20, dtype=jnp.int32)
    distinct = scores * choices_count + jnp.arange(choices_count, dtype=jnp.int32)
    return jnp.argsort(distinct, axis=-1)[..., :NB].astype(jnp.int32)


def with_ends(drawn, own_key, low, top_value):
    spot = [jax.random.randint(jax.random.fold_in(own_key, axis), (), 0, length) for axis, length in enumerate(drawn.shape)]
    main_axis = drawn.shape.index(max(drawn.shape))
    neighbour = spot[:main_axis] + [(spot[main_axis] + 1) % drawn.shape[main_axis]] + spot[main_axis + 1:]
    return drawn.at[tuple(spot)].set(low).at[tuple(neighbour)].set(top_value)


def level_of(stream_key, dims, cuts, smallest, top_value):
    gain, own = 1.0, jax.random.fold_in(stream_key, 6)
    for axis_at, shards_of in cuts:
        draws = jnp.exp(jax.random.uniform(jax.random.fold_in(own, axis_at), (shards_of,), jnp.float32, smallest / len(cuts), top_value / len(cuts)))
        gain = gain * jnp.repeat(draws, dims[axis_at] // shards_of).reshape([-1 if axis == axis_at else 1 for axis in range(len(dims))])
    return gain


def setup_inputs(seed: int = 0) -> dict:
    streams_of = jax.random.split(jax.random.key(seed), 5)
    coords = draw_coords(jax.random.fold_in(streams_of[4], 71), 0)
    masses = jnp.clip(jnp.exp(math.log(2.0) - 1.3862944 * jax.random.uniform(streams_of[1], (CHAN_SLABS, WALL_SLABS, PART), jnp.float32) ** level_of(streams_of[1], (CHAN_SLABS, WALL_SLABS, PART), ((0, 64), (1, 8)), -0.2, 0.2)), 0.5, 2.0)
    counts = with_ends(jax.random.randint(streams_of[2], (CHAN_SLABS, WALL_SLABS, TILE_DEV), TILE // 4, TILE + 1), jax.random.fold_in(streams_of[2], 1), TILE // 4, TILE).astype(jnp.int32)
    lists = draw_lists(jax.random.fold_in(streams_of[4], 71), 0)
    return dict(coords=coords, masses=masses, counts=counts, lists=lists)


def spline(scaled):
    return (jnp.maximum(2.0 - scaled, 0.0) ** 3 * 0.25 - jnp.maximum(1.0 - scaled, 0.0) ** 3) * (1.0 / math.pi)

def pair_block(own_block, partner, partner_rows, offset):
    tile_count = own_block.shape[1]
    tile_len = own_block.shape[2]
    list_len = partner_rows.shape[1]
    picked = jnp.take(partner, partner_rows.reshape(-1), axis=1).reshape(4, tile_count, list_len, tile_len)
    wall_lift = (partner_rows // tile_count - 1).astype(jnp.float32) * (2.0 * R)
    reach = float(R)

    def single_tile(inputs):
        own_tile, theirs, shift_y = inputs
        delta_x = own_tile[0][None, :, None] - (theirs[0][:, None, :] + offset)
        delta_y = own_tile[1][None, :, None] - (theirs[1][:, None, :] + shift_y[:, None, None])
        delta_z = own_tile[2][None, :, None] - theirs[2][:, None, :]
        distance = jnp.sqrt(delta_x * delta_x + delta_y * delta_y + delta_z * delta_z + 0.0001)
        weight = spline(distance / reach)
        gained = lax.optimization_barrier(jnp.sum(weight * theirs[3][:, None, :], axis=(0, 2)))
        handed = lax.optimization_barrier(jnp.sum(weight * own_tile[3][None, :, None], axis=1))
        return (gained, handed)
    gained, handed = lax.map(single_tile, (jnp.moveaxis(own_block, 1, 0), jnp.moveaxis(picked, 1, 0), wall_lift))
    onehot = (partner_rows.reshape(-1)[:, None] == jnp.arange(partner.shape[1], dtype=jnp.int32)[None, :]).astype(jnp.float32)
    returned = jnp.dot(onehot.T, handed.reshape(-1, tile_len), precision=lax.Precision.HIGHEST)
    return (gained, returned)

def reference(coords, masses, counts, lists):
    tile_count = counts.shape[2]
    tile_len = masses.shape[2] // tile_count
    slots = jnp.arange(tile_len, dtype=jnp.int32)
    filled = (slots[None, None, None, :] < counts[..., None]).astype(jnp.float32)
    weighted = masses.reshape(filled.shape) * filled
    packed = jnp.concatenate([coords.reshape(3, CHAN_SLABS, WALL_SLABS, tile_count, tile_len), weighted[None]], axis=0)
    padded = jnp.pad(packed, ((0, 0), (0, 0), (1, 1), (0, 0), (0, 0)))
    extended = jnp.concatenate([padded[:, :, 0:WALL_SLABS], padded[:, :, 1:WALL_SLABS + 1], padded[:, :, 2:]], axis=3)
    flat_own = jnp.moveaxis(packed.reshape(4, -1, tile_count, tile_len), 1, 0)
    density = jnp.zeros((CHAN_SLABS, WALL_SLABS, tile_count, tile_len), jnp.float32)
    returns = jnp.zeros((CHAN_SLABS, WALL_SLABS, 3 * tile_count, tile_len), jnp.float32)
    for step in range(R + 1):
        partner = jnp.roll(extended, -step, axis=1)
        flat_partner = jnp.moveaxis(partner.reshape(4, -1, 3 * tile_count, tile_len), 1, 0)
        flat_lists = lists[:, :, step].reshape(-1, tile_count, NB)

        def per_device(inputs, offset=float(step)):
            return pair_block(inputs[0], inputs[1], inputs[2], offset)
        gained, handed = lax.map(per_device, (flat_own, flat_partner, flat_lists))
        density = density + gained.reshape(CHAN_SLABS, WALL_SLABS, tile_count, tile_len)
        if step > 0:
            returns = returns + jnp.roll(handed.reshape(CHAN_SLABS, WALL_SLABS, 3 * tile_count, tile_len), step, axis=0)
    lower = returns[:, :, :tile_count]
    center = returns[:, :, tile_count:2 * tile_count]
    upper = returns[:, :, 2 * tile_count:]
    from_below = jnp.pad(upper, ((0, 0), (1, 0), (0, 0), (0, 0)))[:, :WALL_SLABS]
    from_above = jnp.pad(lower, ((0, 0), (0, 1), (0, 0), (0, 0)))[:, 1:]
    total = density + center + from_below + from_above
    return (total * filled / (NB * tile_len)).reshape(CHAN_SLABS, WALL_SLABS, -1)
```

```python
import functools
import math

import jax
import jax.numpy as jnp
from jax import lax
from jax.experimental import pallas as pl
from jax.experimental.pallas import tpu as pltpu
from jax.sharding import PartitionSpec as P

R = 4
TILES = 16
TILE = 256
ROWS = 32
EPS = 0.0001 / (R * R)
CHUNK = 32
F32 = jnp.float32
BF16 = jnp.bfloat16
MESH = pl.DeviceIdType.MESH


def split3(value):
    high = value.astype(BF16).astype(F32)
    rest = value - high
    mid = rest.astype(BF16).astype(F32)
    low = (rest - mid).astype(BF16).astype(F32)
    return high, mid, low


def rows_a(value):
    h, m, l = split3(value)
    return [h, h, m, m, h, l]


def rows_b(value):
    h, m, l = split3(value)
    return [h, m, h, m, l, h]


def features_a(x, y, z, w):
    one = jnp.ones_like(x)
    norm = x * x + y * y + z * z + EPS
    rows = rows_a(-2.0 * x) + rows_a(-2.0 * y) + rows_a(-2.0 * z)
    rows += list(split3(norm)) + [one] * 3 + rows_a(w)
    return rows + [jnp.zeros_like(x)] * 2


def features_b(x, y, z, w):
    one = jnp.ones_like(x)
    norm = x * x + y * y + z * z
    rows = rows_b(x) + rows_b(y) + rows_b(z)
    rows += [one] * 3 + list(split3(norm)) + rows_b(w)
    return rows + [jnp.zeros_like(x)] * 2


def kernel(
    chan_count,
    wall_count,
    coords_ref,
    mass_ref,
    counts_ref,
    lists_ref,
    out_ref,
    own,
    walls,
    slabs,
    list_v,
    list_s,
    stage,
    feat_b,
    feat_a,
    dots0,
    dots1,
    part_g,
    full_g,
    gained,
    gained_in,
    handed_rows,
    list_row,
    handed,
    handed_in,
    slab_send,
    slab_recv,
    wall_send,
    wall_recv,
    list_send,
    list_recv,
    gain_send,
    gain_recv,
    hand_send,
    hand_recv,
    list_copy,
):
    c = lax.axis_index("chan")
    w = lax.axis_index("wall")
    has_low = w > 0
    has_high = w < wall_count - 1

    def up(k):
        return (lax.rem(c + k, chan_count), w)

    def down(k):
        return (lax.rem(c + chan_count - k, chan_count), w)

    barrier = pltpu.get_barrier_semaphore()
    for k in range(1, R + 1):
        pl.semaphore_signal(barrier, inc=1, device_id=up(k), device_id_type=MESH)
        pl.semaphore_signal(barrier, inc=1, device_id=down(k), device_id_type=MESH)

    @pl.when(has_low)
    def _():
        pl.semaphore_signal(barrier, inc=1, device_id=(c, w - 1), device_id_type=MESH)

    @pl.when(has_high)
    def _():
        pl.semaphore_signal(barrier, inc=1, device_id=(c, w + 1), device_id_type=MESH)

    row_at = lax.broadcasted_iota(jnp.int32, (ROWS, 128), 0)
    lane_at = lax.broadcasted_iota(jnp.int32, (ROWS, 128), 1)
    slot_at = lax.rem(row_at, 2) * 128 + lane_at
    limit = jnp.zeros((ROWS, 128), jnp.int32)
    for t in range(TILES):
        limit = jnp.where(row_at // 2 == t, counts_ref[t], limit)
    filled = (slot_at < limit).astype(F32)
    own[0:32, :] = coords_ref[0:32, :] * (1.0 / R)
    own[32:64, :] = (coords_ref[32:64, :] - R) * (1.0 / R)
    own[64:96, :] = (coords_ref[64:96, :] - R) * (1.0 / R)
    own[96:128, :] = mass_ref[...] * filled
    full_g[...] = jnp.zeros_like(full_g)
    list_row[...] = jnp.zeros_like(list_row)

    pl.semaphore_wait(barrier, 2 * R + has_low.astype(jnp.int32) + has_high.astype(jnp.int32))

    def wall_copy(slot, target):
        return pltpu.make_async_remote_copy(
            src_ref=own,
            dst_ref=walls.at[slot],
            send_sem=wall_send.at[slot],
            recv_sem=wall_recv.at[slot],
            device_id=(c, target),
            device_id_type=MESH,
        )

    def slab_copy(k):
        return pltpu.make_async_remote_copy(
            src_ref=own,
            dst_ref=slabs.at[k - 1],
            send_sem=slab_send.at[k - 1],
            recv_sem=slab_recv.at[k - 1],
            device_id=up(k),
            device_id_type=MESH,
        )

    def list_send_copy(k):
        return pltpu.make_async_remote_copy(
            src_ref=lists_ref.at[k],
            dst_ref=list_v.at[k],
            send_sem=list_send.at[k - 1],
            recv_sem=list_recv.at[k - 1],
            device_id=up(k),
            device_id_type=MESH,
        )

    def gain_copy(k):
        return pltpu.make_async_remote_copy(
            src_ref=gained.at[k, pl.ds(8, ROWS)],
            dst_ref=gained_in.at[k - 1],
            send_sem=gain_send.at[k - 1],
            recv_sem=gain_recv.at[k - 1],
            device_id=down(k),
            device_id_type=MESH,
        )

    def hand_copy(slot, target):
        return pltpu.make_async_remote_copy(
            src_ref=handed.at[pl.ds(64 * (1 - slot), ROWS)],
            dst_ref=handed_in.at[slot],
            send_sem=hand_send.at[slot],
            recv_sem=hand_recv.at[slot],
            device_id=(c, target),
            device_id_type=MESH,
        )

    @pl.when(has_high)
    def _():
        wall_copy(0, w + 1).start()

    @pl.when(has_low)
    def _():
        wall_copy(1, w - 1).start()

    for k in range(1, R + 1):
        list_send_copy(k).start()
        slab_copy(k).start()

    def stage_rows(rows):
        for f, row in enumerate(rows):
            stage[f * ROWS : (f + 1) * ROWS, :] = row

    feature_at = lax.broadcasted_iota(jnp.int32, (ROWS, 128), 0)

    def build_b(read, side):
        stage_rows(features_b(read(0), read(1) + 2.0 * (side - 1), read(2), read(3)))

        def one(t, carry):
            for half in range(2):
                block = stage[pl.ds(2 * t + half, ROWS, stride=ROWS), :]
                squared = jnp.where(feature_at < 24, block, 0.0).astype(BF16)
                weights = jnp.where(feature_at < 24, 0.0, block).astype(BF16)
                feat_b[side * TILES + t, :, half * 128 : half * 128 + 128] = squared
                feat_b[side * TILES + t, :, 256 + half * 128 : 384 + half * 128] = weights
            return carry

        lax.fori_loop(0, TILES, one, 0)

    def build_a(read, k):
        shift = jnp.asarray(k, jnp.int32).astype(F32) * (1.0 / R)
        stage_rows(features_a(read(0) - shift, read(1), read(2), read(3)))

        def one(t, carry):
            for half in range(2):
                block = stage[pl.ds(2 * t + half, ROWS, stride=ROWS), :]
                feat_a[pl.ds(pl.multiple_of(t * TILE + half * 128, 128), 128), :] = block.T.astype(BF16)
            return carry

        lax.fori_loop(0, TILES, one, 0)

    def own_rows(i):
        return own[32 * i : 32 * i + 32, :]

    build_b(own_rows, 1)

    @pl.when(has_low)
    def _():
        wall_copy(0, w).wait_recv()

    @pl.when(jnp.logical_not(has_low))
    def _():
        walls[0] = jnp.zeros_like(walls[0])

    build_b(lambda i: walls[0, 32 * i : 32 * i + 32, :], 0)

    @pl.when(has_high)
    def _():
        wall_copy(1, w).wait_recv()

    @pl.when(jnp.logical_not(has_high))
    def _():
        walls[1] = jnp.zeros_like(walls[1])

    build_b(lambda i: walls[1, 32 * i : 32 * i + 32, :], 2)

    lane_row = lax.broadcasted_iota(jnp.int32, (1, 128), 1)

    def pair(dots, source, target):
        taken = jnp.zeros((8, TILE), F32)
        for r in range(0, TILE, CHUNK):
            square = dots[r : r + CHUNK, 0:TILE]
            mass = dots[r : r + CHUNK, TILE : 2 * TILE]
            near = 2.0 - square * lax.rsqrt(square)
            outer = near * near * near
            inner = 4.0 - 3.0 * (square * near)
            value = jnp.maximum(jnp.minimum(inner, outer), 0.0) * mass
            row = value[:, 0:128] + value[:, 128:256]
            if source is not None:
                row = row + source[r : r + CHUNK, :]
            target[r : r + CHUNK, :] = row
            for e in range(0, CHUNK, 8):
                taken = taken + value[e : e + 8, :]
        return jnp.sum(taken, axis=0, keepdims=True)

    def section(k, with_back):
        def dot_into(dots, i, n):
            tile = feat_a[pl.ds(pl.multiple_of(i * TILE, TILE), TILE), :]
            j = list_s[k, n, i]
            dots[...] = jnp.dot(tile, feat_b[j], preferred_element_type=F32)

        def flush(i):
            summed = jnp.sum(full_g[...].T, axis=0, keepdims=True)
            gained[k, pl.ds(2 * i + 6, 1), :] = summed[:, 0:128]
            gained[k, pl.ds(2 * i + 7, 1), :] = summed[:, 128:256]

        def note(i, n, row):
            if with_back:
                at = (k - 1) * 32 + 2 * i + n
                handed_rows[pl.ds(at, 1), :] = row
                list_row[...] = jnp.where(lane_row == at, list_s[k, n, i], list_row[...])

        def body(i, carry):
            dot_into(dots1, i, 1)
            flush(i)
            note(i, 0, pair(dots0, None, part_g))
            dot_into(dots0, jnp.minimum(i + 1, TILES - 1), 0)
            note(i, 1, pair(dots1, part_g, full_g))
            return carry

        dot_into(dots0, 0, 0)
        lax.fori_loop(0, TILES, body, 0)
        flush(TILES)

    def far(k, carry):
        list_send_copy(k).wait_recv()
        copy = pltpu.make_async_copy(list_v.at[k], list_s.at[k], list_copy)
        copy.start()
        slab_copy(k).wait_recv()
        build_a(lambda i: slabs[k - 1, 32 * i : 32 * i + 32, :], k)
        copy.wait()
        section(k, True)
        gain_copy(k).start()
        return carry

    lax.fori_loop(1, R + 1, far, 0)

    hot = (lax.broadcasted_iota(jnp.int32, (48, 128), 0) == list_row[...]).astype(F32).astype(BF16)
    summed = jnp.zeros((48, TILE), F32)
    for piece in split3(handed_rows[...]):
        summed = summed + jnp.dot(hot, piece.astype(BF16), preferred_element_type=F32)
    handed[pl.ds(0, 48, stride=2), :] = summed[:, 0:128]
    handed[pl.ds(1, 48, stride=2), :] = summed[:, 128:256]

    copy = pltpu.make_async_copy(lists_ref.at[0], list_s.at[0], list_copy)
    copy.start()
    build_a(own_rows, 0)
    copy.wait()

    @pl.when(has_high)
    def _():
        hand_copy(0, w + 1).start()

    @pl.when(has_low)
    def _():
        hand_copy(1, w - 1).start()

    section(0, False)

    total = gained[0, 8:40, :] + handed[32:64, :]
    for k in range(1, R + 1):
        gain_copy(k).wait_recv()
        total = total + gained_in[k - 1]
    out_ref[...] = total

    @pl.when(has_low)
    def _():
        hand_copy(0, w).wait_recv()
        out_ref[...] += handed_in[0]

    @pl.when(has_high)
    def _():
        hand_copy(1, w).wait_recv()
        out_ref[...] += handed_in[1]

    scale = filled * (1.0 / (4.0 * math.pi * 2 * TILE))
    out_ref[...] = out_ref[...] * scale / mass_ref[...]

    for k in range(1, R + 1):
        slab_copy(k).wait_send()
        list_send_copy(k).wait_send()
        gain_copy(k).wait_send()

    @pl.when(has_high)
    def _():
        wall_copy(0, w).wait_send()
        hand_copy(0, w).wait_send()

    @pl.when(has_low)
    def _():
        wall_copy(1, w).wait_send()
        hand_copy(1, w).wait_send()


def solution(mesh):
    placed = (
        P(None, "chan", "wall", None),
        P("chan", "wall", None),
        P("chan", "wall", None),
        P("chan", "wall", None, None, None),
    )
    chan_count = mesh.shape["chan"]
    wall_count = mesh.shape["wall"]

    def on_device(coords, masses, counts, lists):
        vmem = pl.BlockSpec(memory_space=pltpu.VMEM)
        smem = pl.BlockSpec(memory_space=pltpu.SMEM)
        dma = pltpu.SemaphoreType.DMA
        density = pl.pallas_call(
            functools.partial(kernel, chan_count, wall_count),
            out_shape=jax.ShapeDtypeStruct((ROWS, 128), F32),
            in_specs=[vmem, vmem, smem, vmem],
            out_specs=vmem,
            scratch_shapes=[
                pltpu.VMEM((128, 128), F32),
                pltpu.VMEM((2, 128, 128), F32),
                pltpu.VMEM((R, 128, 128), F32),
                pltpu.VMEM((R + 1, 2, 16), jnp.int32),
                pltpu.SMEM((R + 1, 2, 16), jnp.int32),
                pltpu.VMEM((32 * ROWS, 128), F32),
                pltpu.VMEM((48, 32, 512), BF16),
                pltpu.VMEM((TILES * TILE, 32), BF16),
                pltpu.VMEM((TILE, 512), F32),
                pltpu.VMEM((TILE, 512), F32),
                pltpu.VMEM((TILE, 128), F32),
                pltpu.VMEM((TILE, 128), F32),
                pltpu.VMEM((R + 1, 40, 128), F32),
                pltpu.VMEM((R, ROWS, 128), F32),
                pltpu.VMEM((128, TILE), F32),
                pltpu.VMEM((1, 128), jnp.int32),
                pltpu.VMEM((96, 128), F32),
                pltpu.VMEM((2, ROWS, 128), F32),
                dma((R,)),
                dma((R,)),
                dma((2,)),
                dma((2,)),
                dma((R,)),
                dma((R,)),
                dma((R,)),
                dma((R,)),
                dma((2,)),
                dma((2,)),
                dma(()),
            ],
            compiler_params=pltpu.CompilerParams(collective_id=0, has_side_effects=True),
        )(
            coords.reshape(3 * ROWS, 128),
            masses.reshape(ROWS, 128),
            counts.reshape(TILES),
            jnp.transpose(lists.reshape(R + 1, TILES, 2), (0, 2, 1)),
        )
        return density.reshape(1, 1, -1)

    return jax.shard_map(
        on_device, mesh=mesh, in_specs=placed, out_specs=P("chan", "wall", None), check_vma=False
    )
```

```python
import functools
import math

import jax
import jax.numpy as jnp
from jax import lax
from jax.experimental import pallas as pl
from jax.experimental.pallas import tpu as pltpu
from jax.sharding import PartitionSpec as P

R = 4
TILES = 16
TILE = 256
ROWS = 32
EPS = 0.0001 / (R * R)
CHUNK = 32
UNROLL = 4
FAR = 16.0
F32 = jnp.float32
BF16 = jnp.bfloat16
MESH = pl.DeviceIdType.MESH


def split3(value):
    high = value.astype(BF16).astype(F32)
    rest = value - high
    mid = rest.astype(BF16).astype(F32)
    low = (rest - mid).astype(BF16).astype(F32)
    return high, mid, low


def spread4(value, row):
    swapped = jnp.where(row % 2 == 0, pltpu.roll(value, 7, 1), pltpu.roll(value, 1, 1))
    value = value + swapped
    swapped = jnp.where(row % 4 < 2, pltpu.roll(value, 6, 1), pltpu.roll(value, 2, 1))
    return value + swapped


def halves(first, upper, lower, row):
    upper_turned, lower_turned = pltpu.roll(upper, 4, 1), pltpu.roll(lower, 4, 1)
    top = row < 4
    if first == 0:
        return jnp.where(top, upper, lower_turned)
    return jnp.where(top, upper_turned, lower)


def rows_of(value):
    return lax.broadcasted_iota(jnp.int32, value.shape, 1)


def features_a(packed, shift):
    row = rows_of(packed)
    moved = packed - jnp.where(row % 4 == 0, shift, 0.0)
    coord = row % 4 < 3
    norm = spread4(jnp.where(coord, moved * moved, 0.0), row) + EPS
    high, mid, low = split3(jnp.where(coord, -2.0 * moved, norm))
    mass = split3(spread4(jnp.where(coord, 0.0, packed), row))
    blocks = []
    for half in range(2):
        wide = [halves(half, part, part, row) for part in mass]
        last = jnp.where(row == 3, wide[0], jnp.where(row == 4, wide[1], wide[2]))
        last = jnp.where(row < 3, 1.0, jnp.where(row < 6, last, 0.0))
        blocks.append(
            [
                halves(half, high, high, row),
                halves(half, mid, mid, row),
                halves(half, high, low, row),
                last,
            ]
        )
    return blocks


def features_b(packed, lift):
    row = rows_of(packed)
    coord = row % 4 < 3
    mass = spread4(jnp.where(coord, 0.0, packed), row)
    empty = mass <= 0.0
    mass = jnp.where(empty, 1.0, mass)
    root = jnp.exp(jnp.log(mass) * (1.0 / 3.0))
    root = root - (root * root * root - mass) / (3.0 * root * root)
    square = root * root
    moved = packed + jnp.where(row % 4 == 1, lift, 0.0)
    moved = jnp.where(jnp.logical_and(row % 4 == 2, empty), FAR, moved)
    norm = spread4(jnp.where(coord, moved * moved, 0.0), row) * square
    moved = jnp.where(coord, moved, 1.0) * square
    blocks = []
    parts = []
    for factor in (1.0, 3.0):
        parts.append((split3(factor * moved), split3(factor * norm)))
    for half in range(2):
        block = []
        for (high, mid, low), last in parts:
            last = jnp.where(row % 4 == 0, last[0], jnp.where(row % 4 == 1, last[1], last[2]))
            last = jnp.where(row < 3, halves(half, last, last, row), 0.0)
            mixed = halves(half, high, mid, row)
            block.append([mixed, mixed, halves(half, low, high, row), last])
        block.append(halves(half, 2.0 * root, 2.0 * root, row))
        block.append(halves(half, 4.0 * mass, 4.0 * mass, row))
        blocks.append(block)
    return blocks


def kernel(
    chan_count,
    wall_count,
    coords_ref,
    mass_ref,
    counts_ref,
    lists_ref,
    out_ref,
    walls,
    slabs,
    list_v,
    list_s,
    stage,
    feat_b,
    root_b,
    feat_a,
    dots0,
    dots1,
    mass0,
    mass1,
    part_g,
    full_g,
    gained,
    gained_in,
    handed_rows,
    list_row,
    handed,
    handed_in,
    slab_send,
    slab_recv,
    wall_send,
    wall_recv,
    list_send,
    list_recv,
    gain_send,
    gain_recv,
    hand_send,
    hand_recv,
    list_copy,
):
    c = lax.axis_index("chan")
    w = lax.axis_index("wall")
    has_low = w > 0
    has_high = w < wall_count - 1

    def up(k):
        return (lax.rem(c + k, chan_count), w)

    def down(k):
        return (lax.rem(c + chan_count - k, chan_count), w)

    barrier = pltpu.get_barrier_semaphore()
    for k in range(1, R + 1):
        pl.semaphore_signal(barrier, inc=1, device_id=up(k), device_id_type=MESH)
        pl.semaphore_signal(barrier, inc=1, device_id=down(k), device_id_type=MESH)

    @pl.when(has_low)
    def _():
        pl.semaphore_signal(barrier, inc=1, device_id=(c, w - 1), device_id_type=MESH)

    @pl.when(has_high)
    def _():
        pl.semaphore_signal(barrier, inc=1, device_id=(c, w + 1), device_id_type=MESH)

    row_at = lax.broadcasted_iota(jnp.int32, (ROWS, 128), 0)
    lane_at = lax.broadcasted_iota(jnp.int32, (ROWS, 128), 1)
    slot_at = lax.rem(row_at, 2) * 128 + lane_at
    limit = jnp.zeros((ROWS, 128), jnp.int32)
    for t in range(TILES):
        limit = jnp.where(row_at // 2 == t, counts_ref[t], limit)
    filled = (slot_at < limit).astype(F32)
    own = slabs.at[R]
    own[pl.ds(0, ROWS, stride=4), :] = coords_ref[0:32, :] * (1.0 / R)
    own[pl.ds(1, ROWS, stride=4), :] = (coords_ref[32:64, :] - R) * (1.0 / R)
    own[pl.ds(2, ROWS, stride=4), :] = (coords_ref[64:96, :] - R) * (1.0 / R)
    own[pl.ds(3, ROWS, stride=4), :] = mass_ref[...] * filled
    full_g[...] = jnp.zeros_like(full_g)
    list_row[...] = jnp.zeros_like(list_row)

    pl.semaphore_wait(barrier, 2 * R + has_low.astype(jnp.int32) + has_high.astype(jnp.int32))

    def wall_copy(slot, target):
        return pltpu.make_async_remote_copy(
            src_ref=own,
            dst_ref=walls.at[slot],
            send_sem=wall_send.at[slot],
            recv_sem=wall_recv.at[slot],
            device_id=(c, target),
            device_id_type=MESH,
        )

    def slab_copy(k):
        return pltpu.make_async_remote_copy(
            src_ref=own,
            dst_ref=slabs.at[k - 1],
            send_sem=slab_send.at[k - 1],
            recv_sem=slab_recv.at[k - 1],
            device_id=up(k),
            device_id_type=MESH,
        )

    def list_send_copy(k):
        return pltpu.make_async_remote_copy(
            src_ref=lists_ref.at[k],
            dst_ref=list_v.at[k],
            send_sem=list_send.at[k - 1],
            recv_sem=list_recv.at[k - 1],
            device_id=up(k),
            device_id_type=MESH,
        )

    def gain_copy(k):
        return pltpu.make_async_remote_copy(
            src_ref=gained.at[k, pl.ds(8, ROWS)],
            dst_ref=gained_in.at[k - 1],
            send_sem=gain_send.at[k - 1],
            recv_sem=gain_recv.at[k - 1],
            device_id=down(k),
            device_id_type=MESH,
        )

    def hand_copy(slot, target):
        return pltpu.make_async_remote_copy(
            src_ref=handed.at[pl.ds(64 * (1 - slot), ROWS)],
            dst_ref=handed_in.at[slot],
            send_sem=hand_send.at[slot],
            recv_sem=hand_recv.at[slot],
            device_id=(c, target),
            device_id_type=MESH,
        )

    @pl.when(has_high)
    def _():
        wall_copy(0, w + 1).start()

    @pl.when(has_low)
    def _():
        wall_copy(1, w - 1).start()

    for k in range(1, R + 1):
        list_send_copy(k).start()
        slab_copy(k).start()

    def list_down(k):
        source = list_v.at[k]
        return pltpu.make_async_copy(source, list_s.at[k], list_copy.at[k])

    def own_list_down():
        return pltpu.make_async_copy(lists_ref.at[0], list_s.at[0], list_copy.at[0])

    own_list_down().start()

    def build_b(packed, side):
        blocks = features_b(packed.reshape(TILES, 8, 128), 2.0 * (side - 1))
        tiles = slice(side * TILES, side * TILES + TILES)
        for half, (plain, triple, root, mass) in enumerate(blocks):
            lanes = slice(half * 128, half * 128 + 128)
            for at, rows in ((0, plain), (256, triple)):
                wide = slice(at + half * 128, at + half * 128 + 128)
                for g in range(0, 4, 2):
                    both = jnp.concatenate(rows[g : g + 2], axis=1).astype(BF16)
                    feat_b[tiles, 8 * g : 8 * g + 16, wide] = both
            root_b[tiles, 0:8, lanes] = root
            root_b[tiles, 8:16, lanes] = mass

    def build_a(packed, shift):
        blocks = features_a(packed.reshape(TILES, 8, 128), shift)
        for half in range(2):
            for g in range(4):
                stage[half, :, 8 * g : 8 * g + 8, :] = blocks[half][g]

        def some(s, carry):
            for e in range(4):
                t = 4 * s + e
                for half in range(2):
                    spot = pl.multiple_of(t * TILE + half * 128, 128)
                    feat_a[pl.ds(spot, 128), :] = stage[half, t].T.astype(BF16)
            return carry

        lax.fori_loop(0, TILES // 4, some, 0)

    build_b(own[...], 1)

    @pl.when(has_low)
    def _():
        wall_copy(0, w).wait_recv()

    @pl.when(jnp.logical_not(has_low))
    def _():
        walls[0] = jnp.zeros_like(walls[0])

    build_b(walls[0], 0)

    @pl.when(has_high)
    def _():
        wall_copy(1, w).wait_recv()

    @pl.when(jnp.logical_not(has_high))
    def _():
        walls[1] = jnp.zeros_like(walls[1])

    build_b(walls[1], 2)

    lane_row = lax.broadcasted_iota(jnp.int32, (1, 128), 1)
    pick_at = lax.broadcasted_iota(jnp.int32, (32, 128), 0)
    pick = jnp.logical_and(pick_at >= 27, pick_at < 30).astype(F32).astype(BF16)

    def pair(dots, roots, mass, source, target):
        taken = jnp.zeros((8, TILE), F32)
        root = roots[0:8, :][None]
        top = roots[8:16, :][None]
        for r in range(0, TILE, CHUNK):
            square = dots[r : r + CHUNK, 0:TILE].reshape(CHUNK // 8, 8, TILE)
            triple = dots[r : r + CHUNK, TILE : 2 * TILE].reshape(CHUNK // 8, 8, TILE)
            near = root - square * lax.rsqrt(square)
            outer = near * near * near
            inner = top - triple * near
            value = jnp.maximum(jnp.minimum(inner, outer), 0.0)
            low, high = value[:, :, 0:128], value[:, :, 128:256]
            row = (low + high).reshape(CHUNK, 128)
            if source is not None:
                row = row + source[r : r + CHUNK, :]
            target[r : r + CHUNK, :] = row
            weight = mass[r : r + CHUNK, :].reshape(CHUNK // 8, 8, 128)
            back = jnp.concatenate([low * weight, high * weight], axis=2)
            for e in range(CHUNK // 8):
                taken = taken + back[e]
        return jnp.sum(taken, axis=0, keepdims=True)

    def section(step, k):
        def a_tile(i):
            return feat_a[pl.ds(pl.multiple_of(i * TILE, TILE), TILE), :]

        def dot_into(dots, i, n):
            dots[...] = jnp.dot(a_tile(i), feat_b[list_s[k, n, i]], preferred_element_type=F32)

        def mass_into(mass, i):
            mass[...] = jnp.dot(a_tile(i), pick, preferred_element_type=F32)

        def flush(i):
            summed = jnp.sum(full_g[...].T, axis=0, keepdims=True)
            gained[k, pl.ds(2 * i + 6, 1), :] = summed[:, 0:128]
            gained[k, pl.ds(2 * i + 7, 1), :] = summed[:, 128:256]

        def note(i, n, row):
            at = step * 32 + 2 * i + n
            handed_rows[pl.ds(at, 1), :] = row
            list_row[...] = jnp.where(lane_row == at, list_s[k, n, i], list_row[...])

        masses = (mass0, mass1)

        def body(s, carry):
            for u in range(UNROLL):
                i = s * UNROLL + u
                after = jnp.minimum(i + 1, TILES - 1)
                mass = masses[u % 2]
                dot_into(dots1, i, 1)
                flush(i)
                note(i, 0, pair(dots0, root_b.at[list_s[k, 0, i]], mass, None, part_g))
                dot_into(dots0, after, 0)
                mass_into(masses[(u + 1) % 2], after)
                note(i, 1, pair(dots1, root_b.at[list_s[k, 1, i]], mass, part_g, full_g))
            return carry

        dot_into(dots0, 0, 0)
        mass_into(mass0, 0)
        lax.fori_loop(0, TILES // UNROLL, body, 0)
        flush(TILES)

    list_send_copy(1).wait_recv()
    list_down(1).start()

    def one_offset(step, carry):
        k = lax.rem(step + 1, R + 1)

        @pl.when(step < R - 1)
        def _():
            list_send_copy(k + 1).wait_recv()
            list_down(k + 1).start()

        @pl.when(step < R)
        def _():
            slab_copy(k).wait_recv()
            list_down(k).wait()

        build_a(slabs[step], k.astype(F32) * (1.0 / R))

        @pl.when(step == R)
        def _():
            own_list_down().wait()
            known = list_row[...]
            hot = (lax.broadcasted_iota(jnp.int32, (48, 128), 0) == known).astype(F32).astype(BF16)
            summed = jnp.zeros((48, TILE), F32)
            for piece in split3(handed_rows[0:128, :]):
                summed = summed + jnp.dot(hot, piece.astype(BF16), preferred_element_type=F32)
            handed[pl.ds(0, 48, stride=2), :] = summed[:, 0:128]
            handed[pl.ds(1, 48, stride=2), :] = summed[:, 128:256]

        @pl.when(jnp.logical_and(step == R, has_high))
        def _():
            hand_copy(0, w + 1).start()

        @pl.when(jnp.logical_and(step == R, has_low))
        def _():
            hand_copy(1, w - 1).start()

        section(step, k)

        @pl.when(step < R)
        def _():
            gain_copy(k).start()

        return carry

    lax.fori_loop(0, R + 1, one_offset, 0)

    total = gained[0, 8:40, :]
    for k in range(1, R + 1):
        gain_copy(k).wait_recv()
        total = total + gained_in[k - 1]
    out_ref[...] = handed[32:64, :]

    @pl.when(has_low)
    def _():
        hand_copy(0, w).wait_recv()
        out_ref[...] += handed_in[0]

    @pl.when(has_high)
    def _():
        hand_copy(1, w).wait_recv()
        out_ref[...] += handed_in[1]

    scale = filled * (1.0 / (4.0 * math.pi * 2 * TILE))
    out_ref[...] = (total + out_ref[...] / mass_ref[...]) * scale

    for k in range(1, R + 1):
        slab_copy(k).wait_send()
        list_send_copy(k).wait_send()
        gain_copy(k).wait_send()

    @pl.when(has_high)
    def _():
        wall_copy(0, w).wait_send()
        hand_copy(0, w).wait_send()

    @pl.when(has_low)
    def _():
        wall_copy(1, w).wait_send()
        hand_copy(1, w).wait_send()


def solution(mesh):
    placed = (
        P(None, "chan", "wall", None),
        P("chan", "wall", None),
        P("chan", "wall", None),
        P("chan", "wall", None, None, None),
    )
    chan_count = mesh.shape["chan"]
    wall_count = mesh.shape["wall"]

    def on_device(coords, masses, counts, lists):
        vmem = pl.BlockSpec(memory_space=pltpu.VMEM)
        smem = pl.BlockSpec(memory_space=pltpu.SMEM)
        dma = pltpu.SemaphoreType.DMA
        density = pl.pallas_call(
            functools.partial(kernel, chan_count, wall_count),
            out_shape=jax.ShapeDtypeStruct((ROWS, 128), F32),
            in_specs=[vmem, vmem, smem, vmem],
            out_specs=vmem,
            scratch_shapes=[
                pltpu.VMEM((2, 128, 128), F32),
                pltpu.VMEM((R + 1, 128, 128), F32),
                pltpu.VMEM((R + 1, 2, 16), jnp.int32),
                pltpu.SMEM((R + 1, 2, 16), jnp.int32),
                pltpu.VMEM((2, TILES, 32, 128), F32),
                pltpu.VMEM((48, 32, 512), BF16),
                pltpu.VMEM((48, 16, TILE), F32),
                pltpu.VMEM((TILES * TILE, 32), BF16),
                pltpu.VMEM((TILE, 512), F32),
                pltpu.VMEM((TILE, 512), F32),
                pltpu.VMEM((TILE, 128), F32),
                pltpu.VMEM((TILE, 128), F32),
                pltpu.VMEM((TILE, 128), F32),
                pltpu.VMEM((TILE, 128), F32),
                pltpu.VMEM((R + 1, 40, 128), F32),
                pltpu.VMEM((R, ROWS, 128), F32),
                pltpu.VMEM((32 * (R + 1), TILE), F32),
                pltpu.VMEM((1, 128), jnp.int32),
                pltpu.VMEM((96, 128), F32),
                pltpu.VMEM((2, ROWS, 128), F32),
                dma((R,)),
                dma((R,)),
                dma((2,)),
                dma((2,)),
                dma((R,)),
                dma((R,)),
                dma((R,)),
                dma((R,)),
                dma((2,)),
                dma((2,)),
                dma((R + 1,)),
            ],
            compiler_params=pltpu.CompilerParams(collective_id=0, has_side_effects=True),
        )(
            coords.reshape(3 * ROWS, 128),
            masses.reshape(ROWS, 128),
            counts.reshape(TILES),
            jnp.transpose(lists.reshape(R + 1, TILES, 2), (0, 2, 1)),
        )
        return density.reshape(1, 1, -1)

    return jax.shard_map(
        on_device, mesh=mesh, in_specs=placed, out_specs=P("chan", "wall", None), check_vma=False
    )
```

```python
import functools
import math

import jax
import jax.numpy as jnp
from jax import lax
from jax.experimental import pallas as pl
from jax.experimental.pallas import tpu as pltpu
from jax.sharding import PartitionSpec as P

R = 4
TILES = 16
TILE = 256
ROWS = 32
EPS = 0.0001 / (R * R)
CHUNK = 32
UNROLL = 4
FAR = 16.0
F32 = jnp.float32
BF16 = jnp.bfloat16
MESH = pl.DeviceIdType.MESH


def split3(value):
    high = value.astype(BF16).astype(F32)
    rest = value - high
    mid = rest.astype(BF16).astype(F32)
    low = (rest - mid).astype(BF16).astype(F32)
    return high, mid, low


def spread4(value, row):
    swapped = jnp.where(row % 2 == 0, pltpu.roll(value, 7, 1), pltpu.roll(value, 1, 1))
    value = value + swapped
    swapped = jnp.where(row % 4 < 2, pltpu.roll(value, 6, 1), pltpu.roll(value, 2, 1))
    return value + swapped


def halves(first, upper, lower, row):
    upper_turned, lower_turned = pltpu.roll(upper, 4, 1), pltpu.roll(lower, 4, 1)
    top = row < 4
    if first == 0:
        return jnp.where(top, upper, lower_turned)
    return jnp.where(top, upper_turned, lower)


def rows_of(value):
    return lax.broadcasted_iota(jnp.int32, value.shape, 1)


def features_a(packed, shift):
    row = rows_of(packed)
    moved = packed - jnp.where(row % 4 == 0, shift, 0.0)
    coord = row % 4 < 3
    norm = spread4(jnp.where(coord, moved * moved, 0.0), row) + EPS
    high, mid, low = split3(jnp.where(coord, -2.0 * moved, norm))
    mass = split3(spread4(jnp.where(coord, 0.0, packed), row))
    blocks = []
    for half in range(2):
        wide = [halves(half, part, part, row) for part in mass]
        last = jnp.where(row == 3, wide[0], jnp.where(row == 4, wide[1], wide[2]))
        last = jnp.where(row < 3, 1.0, jnp.where(row < 6, last, 0.0))
        blocks.append(
            [
                halves(half, high, high, row),
                halves(half, mid, mid, row),
                halves(half, high, low, row),
                last,
            ]
        )
    return blocks


def features_b(packed, lift):
    row = rows_of(packed)
    coord = row % 4 < 3
    mass = spread4(jnp.where(coord, 0.0, packed), row)
    empty = mass <= 0.0
    mass = jnp.where(empty, 1.0, mass)
    root = jnp.exp(jnp.log(mass) * (1.0 / 3.0))
    root = root - (root * root * root - mass) / (3.0 * root * root)
    square = root * root
    moved = packed + jnp.where(row % 4 == 1, lift, 0.0)
    moved = jnp.where(jnp.logical_and(row % 4 == 2, empty), FAR, moved)
    norm = spread4(jnp.where(coord, moved * moved, 0.0), row) * square
    moved = jnp.where(coord, moved, 1.0) * square
    blocks = []
    parts = []
    for factor in (1.0, 3.0):
        parts.append((split3(factor * moved), split3(factor * norm)))
    for half in range(2):
        block = []
        for (high, mid, low), last in parts:
            last = jnp.where(row % 4 == 0, last[0], jnp.where(row % 4 == 1, last[1], last[2]))
            last = jnp.where(row < 3, halves(half, last, last, row), 0.0)
            mixed = halves(half, high, mid, row)
            block.append([mixed, mixed, halves(half, low, high, row), last])
        block.append(halves(half, 2.0 * root, 2.0 * root, row))
        block.append(halves(half, 4.0 * mass, 4.0 * mass, row))
        blocks.append(block)
    return blocks


def kernel(
    chan_count,
    wall_count,
    coords_ref,
    mass_ref,
    counts_ref,
    lists_ref,
    out_ref,
    walls,
    slabs,
    list_v,
    list_s,
    stage,
    feat_b,
    root_b,
    feat_a,
    dots0,
    dots1,
    mass0,
    mass1,
    part_g,
    full_g,
    gained,
    gained_in,
    handed_rows,
    list_row,
    handed,
    handed_in,
    slab_send,
    slab_recv,
    wall_send,
    wall_recv,
    list_send,
    list_recv,
    gain_send,
    gain_recv,
    hand_send,
    hand_recv,
    list_copy,
):
    c = lax.axis_index("chan")
    w = lax.axis_index("wall")
    has_low = w > 0
    has_high = w < wall_count - 1

    def up(k):
        return (lax.rem(c + k, chan_count), w)

    def down(k):
        return (lax.rem(c + chan_count - k, chan_count), w)

    barrier = pltpu.get_barrier_semaphore()
    for k in range(1, R + 1):
        pl.semaphore_signal(barrier, inc=1, device_id=down(k), device_id_type=MESH)

    @pl.when(has_low)
    def _():
        pl.semaphore_signal(barrier, inc=1, device_id=(c, w - 1), device_id_type=MESH)

    @pl.when(has_high)
    def _():
        pl.semaphore_signal(barrier, inc=1, device_id=(c, w + 1), device_id_type=MESH)

    row_at = lax.broadcasted_iota(jnp.int32, (ROWS, 128), 0)
    lane_at = lax.broadcasted_iota(jnp.int32, (ROWS, 128), 1)
    slot_at = lax.rem(row_at, 2) * 128 + lane_at
    limit = jnp.zeros((ROWS, 128), jnp.int32)
    for t in range(TILES):
        limit = jnp.where(row_at // 2 == t, counts_ref[t], limit)
    filled = (slot_at < limit).astype(F32)
    own = slabs.at[R]
    own[pl.ds(0, ROWS, stride=4), :] = coords_ref[0:32, :] * (1.0 / R)
    own[pl.ds(1, ROWS, stride=4), :] = (coords_ref[32:64, :] - R) * (1.0 / R)
    own[pl.ds(2, ROWS, stride=4), :] = (coords_ref[64:96, :] - R) * (1.0 / R)
    own[pl.ds(3, ROWS, stride=4), :] = mass_ref[...] * filled
    full_g[...] = jnp.zeros_like(full_g)
    list_row[...] = jnp.zeros_like(list_row)

    pl.semaphore_wait(barrier, R + has_low.astype(jnp.int32) + has_high.astype(jnp.int32))

    def wall_copy(slot, target):
        return pltpu.make_async_remote_copy(
            src_ref=own,
            dst_ref=walls.at[slot],
            send_sem=wall_send.at[slot],
            recv_sem=wall_recv.at[slot],
            device_id=(c, target),
            device_id_type=MESH,
        )

    def slab_copy(k):
        return pltpu.make_async_remote_copy(
            src_ref=own,
            dst_ref=slabs.at[k - 1],
            send_sem=slab_send.at[k - 1],
            recv_sem=slab_recv.at[k - 1],
            device_id=up(k),
            device_id_type=MESH,
        )

    def list_send_copy(k):
        return pltpu.make_async_remote_copy(
            src_ref=lists_ref.at[k],
            dst_ref=list_v.at[k],
            send_sem=list_send.at[k - 1],
            recv_sem=list_recv.at[k - 1],
            device_id=up(k),
            device_id_type=MESH,
        )

    def gain_copy(k):
        return pltpu.make_async_remote_copy(
            src_ref=gained.at[k, pl.ds(8, ROWS)],
            dst_ref=gained_in.at[k - 1],
            send_sem=gain_send.at[k - 1],
            recv_sem=gain_recv.at[k - 1],
            device_id=down(k),
            device_id_type=MESH,
        )

    def hand_copy(slot, target):
        return pltpu.make_async_remote_copy(
            src_ref=handed.at[pl.ds(64 * (1 - slot), ROWS)],
            dst_ref=handed_in.at[slot],
            send_sem=hand_send.at[slot],
            recv_sem=hand_recv.at[slot],
            device_id=(c, target),
            device_id_type=MESH,
        )

    @pl.when(has_high)
    def _():
        wall_copy(0, w + 1).start()

    @pl.when(has_low)
    def _():
        wall_copy(1, w - 1).start()

    for k in range(1, R + 1):
        list_send_copy(k).start()
        slab_copy(k).start()

    def list_down(k):
        source = list_v.at[k]
        return pltpu.make_async_copy(source, list_s.at[k], list_copy.at[k])

    def own_list_down():
        return pltpu.make_async_copy(lists_ref.at[0], list_s.at[0], list_copy.at[0])

    own_list_down().start()

    def build_b(packed, side):
        blocks = features_b(packed.reshape(TILES, 8, 128), 2.0 * (side - 1))
        tiles = slice(side * TILES, side * TILES + TILES)
        for half, (plain, triple, root, mass) in enumerate(blocks):
            lanes = slice(half * 128, half * 128 + 128)
            for at, rows in ((0, plain), (256, triple)):
                wide = slice(at + half * 128, at + half * 128 + 128)
                for g in range(0, 4, 2):
                    both = jnp.concatenate(rows[g : g + 2], axis=1).astype(BF16)
                    feat_b[tiles, 8 * g : 8 * g + 16, wide] = both
            root_b[tiles, 0:8, lanes] = root
            root_b[tiles, 8:16, lanes] = mass

    def build_a(packed, shift):
        blocks = features_a(packed.reshape(TILES, 8, 128), shift)
        for half in range(2):
            for g in range(4):
                stage[half, :, 8 * g : 8 * g + 8, :] = blocks[half][g]

        def some(s, carry):
            for e in range(4):
                t = 4 * s + e
                for half in range(2):
                    spot = pl.multiple_of(t * TILE + half * 128, 128)
                    feat_a[pl.ds(spot, 128), :] = stage[half, t].T.astype(BF16)
            return carry

        lax.fori_loop(0, TILES // 4, some, 0)

    build_b(own[...], 1)

    @pl.when(has_low)
    def _():
        wall_copy(0, w).wait_recv()

    @pl.when(jnp.logical_not(has_low))
    def _():
        walls[0] = jnp.zeros_like(walls[0])

    build_b(walls[0], 0)

    @pl.when(has_high)
    def _():
        wall_copy(1, w).wait_recv()

    @pl.when(jnp.logical_not(has_high))
    def _():
        walls[1] = jnp.zeros_like(walls[1])

    build_b(walls[1], 2)

    lane_row = lax.broadcasted_iota(jnp.int32, (1, 128), 1)
    pick_at = lax.broadcasted_iota(jnp.int32, (32, 128), 0)
    pick = jnp.logical_and(pick_at >= 27, pick_at < 30).astype(F32).astype(BF16)

    def pair(dots, roots, mass, source, target):
        taken = jnp.zeros((8, TILE), F32)
        root = roots[0:8, :][None]
        top = roots[8:16, :][None]
        for r in range(0, TILE, CHUNK):
            square = dots[r : r + CHUNK, 0:TILE].reshape(CHUNK // 8, 8, TILE)
            triple = dots[r : r + CHUNK, TILE : 2 * TILE].reshape(CHUNK // 8, 8, TILE)
            near = root - square * lax.rsqrt(square)
            outer = near * near * near
            inner = top - triple * near
            value = jnp.maximum(jnp.minimum(inner, outer), 0.0)
            low, high = value[:, :, 0:128], value[:, :, 128:256]
            row = (low + high).reshape(CHUNK, 128)
            if source is not None:
                row = row + source[r : r + CHUNK, :]
            target[r : r + CHUNK, :] = row
            weight = mass[r : r + CHUNK, :].reshape(CHUNK // 8, 8, 128)
            back = jnp.concatenate([low * weight, high * weight], axis=2)
            for e in range(CHUNK // 8):
                taken = taken + back[e]
        return jnp.sum(taken, axis=0, keepdims=True)

    def section(step, k):
        def a_tile(i):
            return feat_a[pl.ds(pl.multiple_of(i * TILE, TILE), TILE), :]

        def dot_into(dots, i, n):
            dots[...] = jnp.dot(a_tile(i), feat_b[list_s[k, n, i]], preferred_element_type=F32)

        def mass_into(mass, i):
            mass[...] = jnp.dot(a_tile(i), pick, preferred_element_type=F32)

        def flush(i):
            summed = jnp.sum(full_g[...].T, axis=0, keepdims=True)
            gained[k, pl.ds(2 * i + 6, 1), :] = summed[:, 0:128]
            gained[k, pl.ds(2 * i + 7, 1), :] = summed[:, 128:256]

        def note(i, n, row):
            at = step * 32 + 2 * i + n
            handed_rows[pl.ds(at, 1), :] = row
            list_row[...] = jnp.where(lane_row == at - 32, list_s[k, n, i], list_row[...])

        masses = (mass0, mass1)

        def body(s, carry):
            for u in range(UNROLL):
                i = s * UNROLL + u
                after = jnp.minimum(i + 1, TILES - 1)
                mass = masses[u % 2]
                dot_into(dots1, i, 1)
                flush(i)
                note(i, 0, pair(dots0, root_b.at[list_s[k, 0, i]], mass, None, part_g))
                dot_into(dots0, after, 0)
                mass_into(masses[(u + 1) % 2], after)
                note(i, 1, pair(dots1, root_b.at[list_s[k, 1, i]], mass, part_g, full_g))
            return carry

        dot_into(dots0, 0, 0)
        mass_into(mass0, 0)
        lax.fori_loop(0, TILES // UNROLL, body, 0)
        flush(TILES)

    def offset_at(step):
        return jnp.where(step < 2, step, R + 2 - step)

    def one_offset(step, carry):
        k = offset_at(step)

        @pl.when(step > 0)
        def _():
            list_send_copy(k).wait_recv()
            list_down(k).start()
            slab_copy(k).wait_recv()

        build_a(slabs[lax.rem(k + R, R + 1)], k.astype(F32) * (1.0 / R))

        @pl.when(step > 0)
        def _():
            list_down(k).wait()

        @pl.when(step == 0)
        def _():
            own_list_down().wait()

        section(step, k)

        @pl.when(step > 0)
        def _():
            gain_copy(k).start()

        return carry

    lax.fori_loop(0, R + 1, one_offset, 0)

    known = list_row[...]
    hot = (lax.broadcasted_iota(jnp.int32, (48, 128), 0) == known).astype(F32).astype(BF16)
    summed = jnp.zeros((48, TILE), F32)
    for piece in split3(handed_rows[32:160, :]):
        summed = summed + jnp.dot(hot, piece.astype(BF16), preferred_element_type=F32)
    handed[pl.ds(0, 48, stride=2), :] = summed[:, 0:128]
    handed[pl.ds(1, 48, stride=2), :] = summed[:, 128:256]

    @pl.when(has_high)
    def _():
        hand_copy(0, w + 1).start()

    @pl.when(has_low)
    def _():
        hand_copy(1, w - 1).start()

    total = gained[0, 8:40, :]
    for k in range(1, R + 1):
        gain_copy(k).wait_recv()
        total = total + gained_in[k - 1]
    out_ref[...] = handed[32:64, :]

    @pl.when(has_low)
    def _():
        hand_copy(0, w).wait_recv()
        out_ref[...] += handed_in[0]

    @pl.when(has_high)
    def _():
        hand_copy(1, w).wait_recv()
        out_ref[...] += handed_in[1]

    scale = filled * (1.0 / (4.0 * math.pi * 2 * TILE))
    out_ref[...] = (total + out_ref[...] / mass_ref[...]) * scale

    for k in range(1, R + 1):
        slab_copy(k).wait_send()
        list_send_copy(k).wait_send()
        gain_copy(k).wait_send()

    @pl.when(has_high)
    def _():
        wall_copy(0, w).wait_send()
        hand_copy(0, w).wait_send()

    @pl.when(has_low)
    def _():
        wall_copy(1, w).wait_send()
        hand_copy(1, w).wait_send()


def solution(mesh):
    placed = (
        P(None, "chan", "wall", None),
        P("chan", "wall", None),
        P("chan", "wall", None),
        P("chan", "wall", None, None, None),
    )
    chan_count = mesh.shape["chan"]
    wall_count = mesh.shape["wall"]

    def on_device(coords, masses, counts, lists):
        vmem = pl.BlockSpec(memory_space=pltpu.VMEM)
        smem = pl.BlockSpec(memory_space=pltpu.SMEM)
        dma = pltpu.SemaphoreType.DMA
        density = pl.pallas_call(
            functools.partial(kernel, chan_count, wall_count),
            out_shape=jax.ShapeDtypeStruct((ROWS, 128), F32),
            in_specs=[vmem, vmem, smem, vmem],
            out_specs=vmem,
            scratch_shapes=[
                pltpu.VMEM((2, 128, 128), F32),
                pltpu.VMEM((R + 1, 128, 128), F32),
                pltpu.VMEM((R + 1, 2, 16), jnp.int32),
                pltpu.SMEM((R + 1, 2, 16), jnp.int32),
                pltpu.VMEM((2, TILES, 32, 128), F32),
                pltpu.VMEM((48, 32, 512), BF16),
                pltpu.VMEM((48, 16, TILE), F32),
                pltpu.VMEM((TILES * TILE, 32), BF16),
                pltpu.VMEM((TILE, 512), F32),
                pltpu.VMEM((TILE, 512), F32),
                pltpu.VMEM((TILE, 128), F32),
                pltpu.VMEM((TILE, 128), F32),
                pltpu.VMEM((TILE, 128), F32),
                pltpu.VMEM((TILE, 128), F32),
                pltpu.VMEM((R + 1, 40, 128), F32),
                pltpu.VMEM((R, ROWS, 128), F32),
                pltpu.VMEM((32 * (R + 1), TILE), F32),
                pltpu.VMEM((1, 128), jnp.int32),
                pltpu.VMEM((96, 128), F32),
                pltpu.VMEM((2, ROWS, 128), F32),
                dma((R,)),
                dma((R,)),
                dma((2,)),
                dma((2,)),
                dma((R,)),
                dma((R,)),
                dma((R,)),
                dma((R,)),
                dma((2,)),
                dma((2,)),
                dma((R + 1,)),
            ],
            compiler_params=pltpu.CompilerParams(
                collective_id=0,
                has_side_effects=True,
            ),
        )(
            coords.reshape(3 * ROWS, 128),
            masses.reshape(ROWS, 128),
            counts.reshape(TILES),
            jnp.transpose(lists.reshape(R + 1, TILES, 2), (0, 2, 1)),
        )
        return density.reshape(1, 1, -1)

    return jax.shard_map(
        on_device, mesh=mesh, in_specs=placed, out_specs=P("chan", "wall", None), check_vma=False
    )
```

```python
import functools
import math

import jax
import jax.numpy as jnp
from jax import lax
from jax.experimental import pallas as pl
from jax.experimental.pallas import tpu as pltpu
from jax.sharding import PartitionSpec as P

R = 4
TILES = 16
TILE = 256
ROWS = 32
EPS = 0.0001 / (R * R)
CHUNK = 32
SPLIT = 8
FAR = 16.0
F32 = jnp.float32
BF16 = jnp.bfloat16
MESH = pl.DeviceIdType.MESH


def split3(value):
    high = value.astype(BF16).astype(F32)
    rest = value - high
    mid = rest.astype(BF16).astype(F32)
    low = (rest - mid).astype(BF16).astype(F32)
    return high, mid, low


def spread4(value, row):
    swapped = jnp.where(row % 2 == 0, pltpu.roll(value, 7, 1), pltpu.roll(value, 1, 1))
    value = value + swapped
    swapped = jnp.where(row % 4 < 2, pltpu.roll(value, 6, 1), pltpu.roll(value, 2, 1))
    return value + swapped


def halves(first, upper, lower, row):
    upper_turned, lower_turned = pltpu.roll(upper, 4, 1), pltpu.roll(lower, 4, 1)
    top = row < 4
    if first == 0:
        return jnp.where(top, upper, lower_turned)
    return jnp.where(top, upper_turned, lower)


def rows_of(value):
    return lax.broadcasted_iota(jnp.int32, value.shape, 1)


def features_a(packed, shift):
    row = rows_of(packed)
    moved = packed - jnp.where(row % 4 == 0, shift, 0.0)
    coord = row % 4 < 3
    norm = spread4(jnp.where(coord, moved * moved, 0.0), row) + EPS
    high, mid, low = split3(jnp.where(coord, -2.0 * moved, norm))
    mass = split3(spread4(jnp.where(coord, 0.0, packed), row))
    blocks = []
    for half in range(2):
        wide = [halves(half, part, part, row) for part in mass]
        last = jnp.where(row == 3, wide[0], jnp.where(row == 4, wide[1], wide[2]))
        last = jnp.where(row < 3, 1.0, jnp.where(row < 6, last, 0.0))
        blocks.append(
            [
                halves(half, high, high, row),
                halves(half, mid, mid, row),
                halves(half, high, low, row),
                last,
            ]
        )
    return blocks


def features_b(packed, lift):
    row = rows_of(packed)
    coord = row % 4 < 3
    mass = spread4(jnp.where(coord, 0.0, packed), row)
    empty = mass <= 0.0
    mass = jnp.where(empty, 1.0, mass)
    root = jnp.exp(jnp.log(mass) * (1.0 / 3.0))
    root = root - (root * root * root - mass) / (3.0 * root * root)
    square = root * root
    moved = packed + jnp.where(row % 4 == 1, lift, 0.0)
    moved = jnp.where(jnp.logical_and(row % 4 == 2, empty), FAR, moved)
    norm = spread4(jnp.where(coord, moved * moved, 0.0), row) * square
    moved = jnp.where(coord, moved, 1.0) * square
    blocks = []
    parts = []
    for factor in (1.0, 3.0):
        parts.append((split3(factor * moved), split3(factor * norm)))
    for half in range(2):
        block = []
        for (high, mid, low), last in parts:
            last = jnp.where(row % 4 == 0, last[0], jnp.where(row % 4 == 1, last[1], last[2]))
            last = jnp.where(row < 3, halves(half, last, last, row), 0.0)
            mixed = halves(half, high, mid, row)
            block.append([mixed, mixed, halves(half, low, high, row), last])
        block.append(halves(half, 2.0 * root, 2.0 * root, row))
        block.append(halves(half, 4.0 * mass, 4.0 * mass, row))
        blocks.append(block)
    return blocks


def kernel(
    chan_count,
    wall_count,
    coords_ref,
    mass_ref,
    counts_ref,
    lists_ref,
    out_ref,
    walls,
    slabs,
    list_v,
    list_s,
    stage,
    feat_b,
    root_b,
    feat_a,
    feat_own,
    dots0,
    dots1,
    mass0,
    mass1,
    part_g,
    full_g,
    gained,
    gained_in,
    handed_rows,
    list_row,
    handed,
    handed_in,
    slab_send,
    slab_recv,
    wall_send,
    wall_recv,
    list_send,
    list_recv,
    gain_send,
    gain_recv,
    hand_send,
    hand_recv,
    list_copy,
):
    c = lax.axis_index("chan")
    w = lax.axis_index("wall")
    has_low = w > 0
    has_high = w < wall_count - 1

    def up(k):
        return (lax.rem(c + k, chan_count), w)

    def down(k):
        return (lax.rem(c + chan_count - k, chan_count), w)

    first = lax.rem(c, 2) == 0
    partner = (c + 1 - 2 * lax.rem(c, 2), w)
    barrier = pltpu.get_barrier_semaphore()
    pl.semaphore_signal(barrier, inc=1, device_id=down(2), device_id_type=MESH)
    pl.semaphore_signal(barrier, inc=1, device_id=partner, device_id_type=MESH)

    @pl.when(has_low)
    def _():
        pl.semaphore_signal(barrier, inc=1, device_id=(c, w - 1), device_id_type=MESH)

    @pl.when(has_high)
    def _():
        pl.semaphore_signal(barrier, inc=1, device_id=(c, w + 1), device_id_type=MESH)

    row_at = lax.broadcasted_iota(jnp.int32, (ROWS, 128), 0)
    lane_at = lax.broadcasted_iota(jnp.int32, (ROWS, 128), 1)
    slot_at = lax.rem(row_at, 2) * 128 + lane_at
    limit = jnp.zeros((ROWS, 128), jnp.int32)
    for t in range(TILES):
        limit = jnp.where(row_at // 2 == t, counts_ref[t], limit)
    filled = (slot_at < limit).astype(F32)
    own = slabs.at[R]
    own[pl.ds(0, ROWS, stride=4), :] = coords_ref[0:32, :] * (1.0 / R)
    own[pl.ds(1, ROWS, stride=4), :] = (coords_ref[32:64, :] - R) * (1.0 / R)
    own[pl.ds(2, ROWS, stride=4), :] = (coords_ref[64:96, :] - R) * (1.0 / R)
    own[pl.ds(3, ROWS, stride=4), :] = mass_ref[...] * filled
    list_row[...] = jnp.zeros_like(list_row)
    list_v[R] = lists_ref[...]

    pl.semaphore_wait(barrier, 2 + has_low.astype(jnp.int32) + has_high.astype(jnp.int32))

    def wall_copy(slot, target):
        return pltpu.make_async_remote_copy(
            src_ref=own,
            dst_ref=walls.at[slot],
            send_sem=wall_send.at[slot],
            recv_sem=wall_recv.at[slot],
            device_id=(c, target),
            device_id_type=MESH,
        )

    def pass_on(source, k, target):
        slab = pltpu.make_async_remote_copy(
            src_ref=slabs.at[source],
            dst_ref=slabs.at[k - 1],
            send_sem=slab_send.at[k - 1],
            recv_sem=slab_recv.at[k - 1],
            device_id=target,
            device_id_type=MESH,
        )
        rows = pltpu.make_async_remote_copy(
            src_ref=list_v.at[source],
            dst_ref=list_v.at[k - 1],
            send_sem=list_send.at[k - 1],
            recv_sem=list_recv.at[k - 1],
            device_id=target,
            device_id_type=MESH,
        )
        return slab, rows

    def send(source, k, target):
        slab, rows = pass_on(source, k, target)
        rows.start()
        slab.start()

    def gain_copy(k):
        return pltpu.make_async_remote_copy(
            src_ref=gained.at[k],
            dst_ref=gained_in.at[k - 1],
            send_sem=gain_send.at[k - 1],
            recv_sem=gain_recv.at[k - 1],
            device_id=down(k),
            device_id_type=MESH,
        )

    def hand_copy(slot, target):
        return pltpu.make_async_remote_copy(
            src_ref=handed.at[pl.ds(64 * (1 - slot), ROWS)],
            dst_ref=handed_in.at[slot],
            send_sem=hand_send.at[slot],
            recv_sem=hand_recv.at[slot],
            device_id=(c, target),
            device_id_type=MESH,
        )

    @pl.when(has_high)
    def _():
        wall_copy(0, w + 1).start()

    @pl.when(has_low)
    def _():
        wall_copy(1, w - 1).start()

    send(R, 2, up(2))

    @pl.when(first)
    def _():
        send(R, 1, partner)

    def list_down(k):
        return pltpu.make_async_copy(list_v.at[k - 1, k], list_s.at[k], list_copy.at[k])

    def own_list_down():
        return pltpu.make_async_copy(lists_ref.at[0], list_s.at[0], list_copy.at[0])

    own_list_down().start()

    def build_b(packed, side):
        blocks = features_b(packed.reshape(TILES, 8, 128), 2.0 * (side - 1))
        tiles = slice(side * TILES, side * TILES + TILES)
        for half, (plain, triple, root, mass) in enumerate(blocks):
            lanes = slice(half * 128, half * 128 + 128)
            for at, rows in ((0, plain), (256, triple)):
                wide = slice(at + half * 128, at + half * 128 + 128)
                for g in range(0, 4, 2):
                    both = jnp.concatenate(rows[g : g + 2], axis=1).astype(BF16)
                    feat_b[tiles, 8 * g : 8 * g + 16, wide] = both
            root_b[tiles, 0:8, lanes] = root
            root_b[tiles, 8:16, lanes] = mass

    def build_a(feat, packed, shift):
        blocks = features_a(packed.reshape(TILES, 8, 128), shift)
        for half in range(2):
            for g in range(4):
                stage[half, :, 8 * g : 8 * g + 8, :] = blocks[half][g]
        for q in range(TILES // 4):
            for half in range(2):
                spot = q * TILE + half * 128
                turned = stage[half, 4 * q : 4 * q + 4].reshape(128, 128).T
                feat[spot : spot + 128, :] = turned.astype(BF16)

    build_a(feat_own, own[...], 0.0)
    build_b(own[...], 1)

    @pl.when(has_low)
    def _():
        wall_copy(0, w).wait_recv()

    @pl.when(jnp.logical_not(has_low))
    def _():
        walls[0] = jnp.zeros_like(walls[0])

    build_b(walls[0], 0)

    @pl.when(has_high)
    def _():
        wall_copy(1, w).wait_recv()

    @pl.when(jnp.logical_not(has_high))
    def _():
        walls[1] = jnp.zeros_like(walls[1])

    build_b(walls[1], 2)

    lane_row = lax.broadcasted_iota(jnp.int32, (1, 128), 1)
    pick_at = lax.broadcasted_iota(jnp.int32, (32, 128), 0)
    pick = jnp.logical_and(pick_at >= 27, pick_at < 30).astype(F32).astype(BF16)

    def placed(rows, quarter):
        width = rows.shape[1]
        parts = [jnp.zeros((32 * quarter, width), BF16)] if quarter else []
        parts.append(rows)
        if quarter < 3:
            parts.append(jnp.zeros((96 - 32 * quarter, width), BF16))
        return jnp.concatenate(parts, axis=0)


    def pair(dots, roots, mass, source, target):
        taken = jnp.zeros((8, TILE), F32)
        root = roots[0:8, :][None]
        top = roots[8:16, :][None]
        for r in range(0, TILE, CHUNK):
            square = dots[r : r + CHUNK, 0:TILE].reshape(CHUNK // 8, 8, TILE)
            triple = dots[r : r + CHUNK, TILE : 2 * TILE].reshape(CHUNK // 8, 8, TILE)
            near = root - square * lax.rsqrt(square)
            outer = near * near * near
            inner = top - triple * near
            value = lax.clamp(jnp.zeros_like(inner), outer, inner)
            low, high = value[:, :, 0:128], value[:, :, 128:256]
            row = (low + high).reshape(CHUNK, 128)
            if source is not None:
                row = row + source[r : r + CHUNK, :]
            target[r : r + CHUNK, :] = row
            weight = mass[r : r + CHUNK, :].reshape(CHUNK // 8, 8, 128)
            back = jnp.concatenate([low * weight, high * weight], axis=2)
            for e in range(CHUNK // 8):
                taken = taken + back[e]
        return jnp.sum(taken, axis=0, keepdims=True)

    def section(step, k, feat, begin, end):
        def a_tile(i):
            return feat[(i // 4) * TILE : (i // 4) * TILE + TILE, :]

        def dot_into(dots, i, n):
            rows = placed(feat_b[list_s[k, n, i]], i % 4)
            dots[...] = jnp.dot(a_tile(i), rows, preferred_element_type=F32)

        def mass_into(mass, i):
            mass[...] = jnp.dot(a_tile(i), placed(pick, i % 4), preferred_element_type=F32)

        def flush(i):
            summed = jnp.sum(full_g[...].T, axis=0, keepdims=True)
            gained[k, 2 * i : 2 * i + 1, :] = summed[:, 0:128]
            gained[k, 2 * i + 1 : 2 * i + 2, :] = summed[:, 128:256]

        def note(i, n, row):
            if step is not None:
                at = step * 32 + 2 * i + n
                handed_rows[pl.ds(at, 1), :] = row
                list_row[...] = jnp.where(lane_row == at, list_s[k, n, i], list_row[...])

        masses = (mass0, mass1)
        dot_into(dots0, begin, 0)
        mass_into(mass0, begin)
        for i in range(begin, end):
            mass = masses[(i - begin) % 2]
            dot_into(dots1, i, 1)
            if i > begin:
                flush(i - 1)
            note(i, 0, pair(dots0, root_b.at[list_s[k, 0, i]], mass, None, part_g))
            if i + 1 < end:
                dot_into(dots0, i + 1, 0)
                mass_into(masses[(i + 1 - begin) % 2], i + 1)
            note(i, 1, pair(dots1, root_b.at[list_s[k, 1, i]], mass, part_g, full_g))
        flush(end - 1)

    own_list_down().wait()
    section(None, 0, feat_own, 0, SPLIT)

    def one_offset(step, carry):
        k = jnp.where(step < 2, 2 * step + 2, 7 - 2 * step)
        slab, rows = pass_on(R, k, partner)
        rows.wait_recv()
        list_down(k).start()
        slab.wait_recv()

        @pl.when(step == 0)
        def _():
            send(1, 4, up(2))

        @pl.when(jnp.logical_and(step == 0, first))
        def _():
            send(1, 3, partner)

        @pl.when(jnp.logical_and(step == 0, jnp.logical_not(first)))
        def _():
            send(1, 1, partner)

        @pl.when(jnp.logical_and(step == 1, jnp.logical_not(first)))
        def _():
            send(3, 3, partner)

        build_a(feat_a, slabs[k - 1], k.astype(F32) * (1.0 / R))
        list_down(k).wait()
        section(step, k, feat_a, 0, TILES)
        gain_copy(k).start()
        return carry

    lax.fori_loop(0, R, one_offset, 0)

    known = list_row[...]
    hot = (lax.broadcasted_iota(jnp.int32, (48, 128), 0) == known).astype(F32).astype(BF16)
    summed = jnp.zeros((48, TILE), F32)
    for piece in split3(handed_rows[...]):
        summed = summed + jnp.dot(hot, piece.astype(BF16), preferred_element_type=F32)
    handed[pl.ds(0, 48, stride=2), :] = summed[:, 0:128]
    handed[pl.ds(1, 48, stride=2), :] = summed[:, 128:256]

    @pl.when(has_high)
    def _():
        hand_copy(0, w + 1).start()

    @pl.when(has_low)
    def _():
        hand_copy(1, w - 1).start()

    section(None, 0, feat_own, SPLIT, TILES)

    total = gained[0]
    for k in range(1, R + 1):
        gain_copy(k).wait_recv()
        total = total + gained_in[k - 1]
    out_ref[...] = handed[32:64, :]

    @pl.when(has_low)
    def _():
        hand_copy(0, w).wait_recv()
        out_ref[...] += handed_in[0]

    @pl.when(has_high)
    def _():
        hand_copy(1, w).wait_recv()
        out_ref[...] += handed_in[1]

    scale = filled * (1.0 / (4.0 * math.pi * 2 * TILE))
    out_ref[...] = (total + out_ref[...] / mass_ref[...]) * scale

    for k in range(1, R + 1):
        slab, rows = pass_on(R, k, partner)
        slab.wait_send()
        rows.wait_send()
        gain_copy(k).wait_send()

    @pl.when(has_high)
    def _():
        wall_copy(0, w).wait_send()
        hand_copy(0, w).wait_send()

    @pl.when(has_low)
    def _():
        wall_copy(1, w).wait_send()
        hand_copy(1, w).wait_send()


def solution(mesh):
    placed = (
        P(None, "chan", "wall", None),
        P("chan", "wall", None),
        P("chan", "wall", None),
        P("chan", "wall", None, None, None),
    )
    chan_count = mesh.shape["chan"]
    wall_count = mesh.shape["wall"]

    def on_device(coords, masses, counts, lists):
        vmem = pl.BlockSpec(memory_space=pltpu.VMEM)
        smem = pl.BlockSpec(memory_space=pltpu.SMEM)
        dma = pltpu.SemaphoreType.DMA
        density = pl.pallas_call(
            functools.partial(kernel, chan_count, wall_count),
            out_shape=jax.ShapeDtypeStruct((ROWS, 128), F32),
            in_specs=[vmem, vmem, smem, vmem],
            out_specs=vmem,
            scratch_shapes=[
                pltpu.VMEM((2, 128, 128), F32),
                pltpu.VMEM((R + 1, 128, 128), F32),
                pltpu.VMEM((R + 1, R + 1, 2, 16), jnp.int32),
                pltpu.SMEM((R + 1, 2, 16), jnp.int32),
                pltpu.VMEM((2, TILES, 32, 128), F32),
                pltpu.VMEM((48, 32, 512), BF16),
                pltpu.VMEM((48, 16, TILE), F32),
                pltpu.VMEM((4 * TILE, 128), BF16),
                pltpu.VMEM((4 * TILE, 128), BF16),
                pltpu.VMEM((TILE, 512), F32),
                pltpu.VMEM((TILE, 512), F32),
                pltpu.VMEM((TILE, 128), F32),
                pltpu.VMEM((TILE, 128), F32),
                pltpu.VMEM((TILE, 128), F32),
                pltpu.VMEM((TILE, 128), F32),
                pltpu.VMEM((R + 1, ROWS, 128), F32),
                pltpu.VMEM((R, ROWS, 128), F32),
                pltpu.VMEM((32 * R, TILE), F32),
                pltpu.VMEM((1, 128), jnp.int32),
                pltpu.VMEM((96, 128), F32),
                pltpu.VMEM((2, ROWS, 128), F32),
                dma((R,)),
                dma((R,)),
                dma((2,)),
                dma((2,)),
                dma((R,)),
                dma((R,)),
                dma((R,)),
                dma((R,)),
                dma((2,)),
                dma((2,)),
                dma((R + 1,)),
            ],
            compiler_params=pltpu.CompilerParams(
                collective_id=0,
                has_side_effects=True,
            ),
        )(
            coords.reshape(3 * ROWS, 128),
            masses.reshape(ROWS, 128),
            counts.reshape(TILES),
            jnp.transpose(lists.reshape(R + 1, TILES, 2), (0, 2, 1)),
        )
        return density.reshape(1, 1, -1)

    return jax.shard_map(
        on_device, mesh=mesh, in_specs=placed, out_specs=P("chan", "wall", None), check_vma=False
    )
```

```python
import functools
import math

import jax
import jax.numpy as jnp
from jax import lax
from jax.experimental import pallas as pl
from jax.experimental.pallas import tpu as pltpu
from jax.sharding import PartitionSpec as P

R = 4
TILES = 16
TILE = 256
ROWS = 32
EPS = 0.0001 / (R * R)
CHUNK = 32
SPLIT = 8
FAR = 16.0
F32 = jnp.float32
BF16 = jnp.bfloat16
MESH = pl.DeviceIdType.MESH


def split3(value):
    high = value.astype(BF16).astype(F32)
    rest = value - high
    mid = rest.astype(BF16).astype(F32)
    low = (rest - mid).astype(BF16).astype(F32)
    return high, mid, low


def spread4(value, row):
    swapped = jnp.where(row % 2 == 0, pltpu.roll(value, 7, 1), pltpu.roll(value, 1, 1))
    value = value + swapped
    swapped = jnp.where(row % 4 < 2, pltpu.roll(value, 6, 1), pltpu.roll(value, 2, 1))
    return value + swapped


def halves(first, upper, lower, row):
    upper_turned, lower_turned = pltpu.roll(upper, 4, 1), pltpu.roll(lower, 4, 1)
    top = row < 4
    if first == 0:
        return jnp.where(top, upper, lower_turned)
    return jnp.where(top, upper_turned, lower)


def rows_of(value):
    return lax.broadcasted_iota(jnp.int32, value.shape, 1)


def features_a(packed, shift):
    row = rows_of(packed)
    moved = packed - jnp.where(row % 4 == 0, shift, 0.0)
    coord = row % 4 < 3
    norm = spread4(jnp.where(coord, moved * moved, 0.0), row) + EPS
    high, mid, low = split3(jnp.where(coord, -2.0 * moved, norm))
    mass = split3(spread4(jnp.where(coord, 0.0, packed), row))
    blocks = []
    for half in range(2):
        wide = [halves(half, part, part, row) for part in mass]
        last = jnp.where(row == 3, wide[0], jnp.where(row == 4, wide[1], wide[2]))
        last = jnp.where(row < 3, 1.0, jnp.where(row < 6, last, 0.0))
        blocks.append(
            [
                halves(half, high, high, row),
                halves(half, mid, mid, row),
                halves(half, high, low, row),
                last,
            ]
        )
    return blocks


def features_b(packed, lift):
    row = rows_of(packed)
    coord = row % 4 < 3
    mass = spread4(jnp.where(coord, 0.0, packed), row)
    empty = mass <= 0.0
    mass = jnp.where(empty, 1.0, mass)
    root = jnp.exp(jnp.log(mass) * (1.0 / 3.0))
    root = root - (root * root * root - mass) / (3.0 * root * root)
    square = root * root
    moved = packed + jnp.where(row % 4 == 1, lift, 0.0)
    moved = jnp.where(jnp.logical_and(row % 4 == 2, empty), FAR, moved)
    norm = spread4(jnp.where(coord, moved * moved, 0.0), row) * square
    moved = jnp.where(coord, moved, 1.0) * square
    blocks = []
    parts = []
    for factor in (1.0, 3.0):
        parts.append((split3(factor * moved), split3(factor * norm)))
    for half in range(2):
        block = []
        for (high, mid, low), last in parts:
            last = jnp.where(row % 4 == 0, last[0], jnp.where(row % 4 == 1, last[1], last[2]))
            last = jnp.where(row < 3, halves(half, last, last, row), 0.0)
            mixed = halves(half, high, mid, row)
            block.append([mixed, mixed, halves(half, low, high, row), last])
        block.append(halves(half, 2.0 * root, 2.0 * root, row))
        block.append(halves(half, 4.0 * mass, 4.0 * mass, row))
        blocks.append(block)
    return blocks


def kernel(
    chan_count,
    wall_count,
    coords_hbm,
    mass_hbm,
    counts_hbm,
    lists_hbm,
    out_ref,
    coords_ref,
    mass_ref,
    counts_ref,
    input_sem,
    walls,
    slabs,
    list_v,
    list_s,
    stage,
    feat_b,
    root_b,
    feat_a,
    feat_own,
    dots0,
    dots1,
    mass0,
    mass1,
    part_g,
    full_g,
    gained,
    gained_in,
    handed_rows,
    list_row,
    handed,
    handed_in,
    slab_send,
    slab_recv,
    wall_send,
    wall_recv,
    list_send,
    list_recv,
    gain_send,
    gain_recv,
    hand_send,
    hand_recv,
    list_copy,
):
    c = lax.axis_index("chan")
    w = lax.axis_index("wall")
    has_low = w > 0
    has_high = w < wall_count - 1

    def up(k):
        return (lax.rem(c + k, chan_count), w)

    def down(k):
        return (lax.rem(c + chan_count - k, chan_count), w)

    first = lax.rem(c, 2) == 0
    partner = (c + 1 - 2 * lax.rem(c, 2), w)
    barrier = pltpu.get_barrier_semaphore()
    pl.semaphore_signal(barrier, inc=1, device_id=down(2), device_id_type=MESH)
    pl.semaphore_signal(barrier, inc=1, device_id=partner, device_id_type=MESH)

    @pl.when(has_low)
    def _():
        pl.semaphore_signal(barrier, inc=1, device_id=(c, w - 1), device_id_type=MESH)

    @pl.when(has_high)
    def _():
        pl.semaphore_signal(barrier, inc=1, device_id=(c, w + 1), device_id_type=MESH)

    inputs = [
        pltpu.make_async_copy(source, target, input_sem.at[at])
        for at, (source, target) in enumerate(
            (
                (counts_hbm, counts_ref),
                (coords_hbm, coords_ref),
                (mass_hbm, mass_ref),
                (lists_hbm, list_v.at[R]),
                (lists_hbm.at[0], list_s.at[0]),
            )
        )
    ]
    for copy in inputs:
        copy.start()
    row_at = lax.broadcasted_iota(jnp.int32, (ROWS, 128), 0)
    lane_at = lax.broadcasted_iota(jnp.int32, (ROWS, 128), 1)
    slot_at = lax.rem(row_at, 2) * 128 + lane_at
    limit = jnp.zeros((ROWS, 128), jnp.int32)
    for copy in inputs:
        copy.wait()
    for t in range(TILES):
        limit = jnp.where(row_at // 2 == t, counts_ref[t], limit)
    filled = (slot_at < limit).astype(F32)
    own = slabs.at[R]
    own[pl.ds(0, ROWS, stride=4), :] = coords_ref[0:32, :] * (1.0 / R)
    own[pl.ds(1, ROWS, stride=4), :] = (coords_ref[32:64, :] - R) * (1.0 / R)
    own[pl.ds(2, ROWS, stride=4), :] = (coords_ref[64:96, :] - R) * (1.0 / R)
    own[pl.ds(3, ROWS, stride=4), :] = mass_ref[...] * filled
    list_row[...] = jnp.zeros_like(list_row)

    pl.semaphore_wait(barrier, 2 + has_low.astype(jnp.int32) + has_high.astype(jnp.int32))

    def wall_copy(slot, target):
        return pltpu.make_async_remote_copy(
            src_ref=own,
            dst_ref=walls.at[slot],
            send_sem=wall_send.at[slot],
            recv_sem=wall_recv.at[slot],
            device_id=(c, target),
            device_id_type=MESH,
        )

    def pass_on(source, k, target):
        slab = pltpu.make_async_remote_copy(
            src_ref=slabs.at[source],
            dst_ref=slabs.at[k - 1],
            send_sem=slab_send.at[k - 1],
            recv_sem=slab_recv.at[k - 1],
            device_id=target,
            device_id_type=MESH,
        )
        rows = pltpu.make_async_remote_copy(
            src_ref=list_v.at[source],
            dst_ref=list_v.at[k - 1],
            send_sem=list_send.at[k - 1],
            recv_sem=list_recv.at[k - 1],
            device_id=target,
            device_id_type=MESH,
        )
        return slab, rows

    def send(source, k, target):
        slab, rows = pass_on(source, k, target)
        rows.start()
        slab.start()

    def gain_copy(k):
        return pltpu.make_async_remote_copy(
            src_ref=gained.at[k],
            dst_ref=gained_in.at[k - 1],
            send_sem=gain_send.at[k - 1],
            recv_sem=gain_recv.at[k - 1],
            device_id=down(k),
            device_id_type=MESH,
        )

    def hand_copy(slot, target):
        return pltpu.make_async_remote_copy(
            src_ref=handed.at[pl.ds(64 * (1 - slot), ROWS)],
            dst_ref=handed_in.at[slot],
            send_sem=hand_send.at[slot],
            recv_sem=hand_recv.at[slot],
            device_id=(c, target),
            device_id_type=MESH,
        )

    @pl.when(has_high)
    def _():
        wall_copy(0, w + 1).start()

    @pl.when(has_low)
    def _():
        wall_copy(1, w - 1).start()

    send(R, 2, up(2))

    @pl.when(first)
    def _():
        send(R, 1, partner)

    def list_down(k):
        return pltpu.make_async_copy(list_v.at[k - 1, k], list_s.at[k], list_copy.at[k])

    def build_b(packed, side):
        blocks = features_b(packed.reshape(TILES, 8, 128), 2.0 * (side - 1))
        tiles = slice(side * TILES, side * TILES + TILES)
        for half, (plain, triple, root, mass) in enumerate(blocks):
            lanes = slice(half * 128, half * 128 + 128)
            for at, rows in ((0, plain), (256, triple)):
                wide = slice(at + half * 128, at + half * 128 + 128)
                for g in range(0, 4, 2):
                    both = jnp.concatenate(rows[g : g + 2], axis=1).astype(BF16)
                    feat_b[tiles, 8 * g : 8 * g + 16, wide] = both
            root_b[tiles, 0:8, lanes] = root
            root_b[tiles, 8:16, lanes] = mass

    def build_a(feat, packed, shift):
        blocks = features_a(packed.reshape(TILES, 8, 128), shift)
        for half in range(2):
            for g in range(4):
                stage[half, :, 8 * g : 8 * g + 8, :] = blocks[half][g]
        for q in range(TILES // 4):
            for half in range(2):
                spot = q * TILE + half * 128
                turned = stage[half, 4 * q : 4 * q + 4].reshape(128, 128).T
                feat[spot : spot + 128, :] = turned.astype(BF16)

    build_a(feat_own, own[...], 0.0)
    build_b(own[...], 1)

    @pl.when(has_low)
    def _():
        wall_copy(0, w).wait_recv()

    @pl.when(jnp.logical_not(has_low))
    def _():
        walls[0] = jnp.zeros_like(walls[0])

    build_b(walls[0], 0)

    @pl.when(has_high)
    def _():
        wall_copy(1, w).wait_recv()

    @pl.when(jnp.logical_not(has_high))
    def _():
        walls[1] = jnp.zeros_like(walls[1])

    build_b(walls[1], 2)

    lane_row = lax.broadcasted_iota(jnp.int32, (1, 128), 1)
    pick_at = lax.broadcasted_iota(jnp.int32, (32, 128), 0)
    pick = jnp.logical_and(pick_at >= 27, pick_at < 30).astype(F32).astype(BF16)

    def placed(rows, quarter):
        width = rows.shape[1]
        parts = [jnp.zeros((32 * quarter, width), BF16)] if quarter else []
        parts.append(rows)
        if quarter < 3:
            parts.append(jnp.zeros((96 - 32 * quarter, width), BF16))
        return jnp.concatenate(parts, axis=0)


    def pair(dots, roots, mass, source, target):
        taken = jnp.zeros((8, TILE), F32)
        root = roots[0:8, :][None]
        top = roots[8:16, :][None]
        for r in range(0, TILE, CHUNK):
            square = dots[r : r + CHUNK, 0:TILE].reshape(CHUNK // 8, 8, TILE)
            triple = dots[r : r + CHUNK, TILE : 2 * TILE].reshape(CHUNK // 8, 8, TILE)
            near = root - square * lax.rsqrt(square)
            outer = near * near * near
            inner = top - triple * near
            value = lax.clamp(jnp.zeros_like(inner), outer, inner)
            low, high = value[:, :, 0:128], value[:, :, 128:256]
            row = (low + high).reshape(CHUNK, 128)
            if source is not None:
                row = row + source[r : r + CHUNK, :]
            target[r : r + CHUNK, :] = row
            weight = mass[r : r + CHUNK, :].reshape(CHUNK // 8, 8, 128)
            back = jnp.concatenate([low * weight, high * weight], axis=2)
            for e in range(CHUNK // 8):
                taken = taken + back[e]
        return jnp.sum(taken, axis=0, keepdims=True)

    def section(step, k, feat, begin, end):
        def a_tile(i):
            return feat[(i // 4) * TILE : (i // 4) * TILE + TILE, :]

        def dot_into(dots, i, n):
            rows = placed(feat_b[list_s[k, n, i]], i % 4)
            dots[...] = jnp.dot(a_tile(i), rows, preferred_element_type=F32)

        def mass_into(mass, i):
            mass[...] = jnp.dot(a_tile(i), placed(pick, i % 4), preferred_element_type=F32)

        def flush(i):
            summed = jnp.sum(full_g[...].T, axis=0, keepdims=True)
            gained[k, 2 * i : 2 * i + 1, :] = summed[:, 0:128]
            gained[k, 2 * i + 1 : 2 * i + 2, :] = summed[:, 128:256]

        def note(i, n, row):
            if step is not None:
                at = step * 32 + 2 * i + n
                handed_rows[pl.ds(at, 1), :] = row
                list_row[...] = jnp.where(lane_row == at, list_s[k, n, i], list_row[...])

        masses = (mass0, mass1)
        dot_into(dots0, begin, 0)
        mass_into(mass0, begin)
        for i in range(begin, end):
            mass = masses[(i - begin) % 2]
            dot_into(dots1, i, 1)
            if i > begin:
                flush(i - 1)
            note(i, 0, pair(dots0, root_b.at[list_s[k, 0, i]], mass, None, part_g))
            if i + 1 < end:
                dot_into(dots0, i + 1, 0)
                mass_into(masses[(i + 1 - begin) % 2], i + 1)
            note(i, 1, pair(dots1, root_b.at[list_s[k, 1, i]], mass, part_g, full_g))
        flush(end - 1)

    late = c < 2

    def take(k):
        slab, rows = pass_on(R, k, partner)
        rows.wait_recv()
        slab.wait_recv()

    def relay():
        take(2)
        send(1, 4, up(2))

        @pl.when(first)
        def _():
            send(1, 3, partner)

        @pl.when(jnp.logical_not(first))
        def _():
            send(1, 1, partner)

    pl.when(jnp.logical_not(late))(relay)
    section(None, 0, feat_own, 0, SPLIT)
    pl.when(late)(relay)

    def one_offset(step, carry):
        k = jnp.where(step < 2, 2 - step, 6 - step)

        @pl.when(step > 0)
        def _():
            take(k)

        list_down(k).start()

        @pl.when(jnp.logical_and(step == 2, jnp.logical_not(first)))
        def _():
            send(3, 3, partner)

        build_a(feat_a, slabs[k - 1], k.astype(F32) * (1.0 / R))
        list_down(k).wait()
        section(step, k, feat_a, 0, TILES)
        gain_copy(k).start()
        return carry

    lax.fori_loop(0, R, one_offset, 0)

    known = list_row[...]
    hot = (lax.broadcasted_iota(jnp.int32, (48, 128), 0) == known).astype(F32).astype(BF16)
    summed = jnp.zeros((48, TILE), F32)
    for piece in split3(handed_rows[...]):
        summed = summed + jnp.dot(hot, piece.astype(BF16), preferred_element_type=F32)
    handed[pl.ds(0, 48, stride=2), :] = summed[:, 0:128]
    handed[pl.ds(1, 48, stride=2), :] = summed[:, 128:256]

    @pl.when(has_high)
    def _():
        hand_copy(0, w + 1).start()

    @pl.when(has_low)
    def _():
        hand_copy(1, w - 1).start()

    section(None, 0, feat_own, SPLIT, TILES)

    total = gained[0]
    for k in range(1, R + 1):
        gain_copy(k).wait_recv()
        total = total + gained_in[k - 1]
    out_ref[...] = handed[32:64, :]

    @pl.when(has_low)
    def _():
        hand_copy(0, w).wait_recv()
        out_ref[...] += handed_in[0]

    @pl.when(has_high)
    def _():
        hand_copy(1, w).wait_recv()
        out_ref[...] += handed_in[1]

    scale = filled * (1.0 / (4.0 * math.pi * 2 * TILE))
    out_ref[...] = (total + out_ref[...] / mass_ref[...]) * scale

    for k in range(1, R + 1):
        slab, rows = pass_on(R, k, partner)
        slab.wait_send()
        rows.wait_send()
        gain_copy(k).wait_send()

    @pl.when(has_high)
    def _():
        wall_copy(0, w).wait_send()
        hand_copy(0, w).wait_send()

    @pl.when(has_low)
    def _():
        wall_copy(1, w).wait_send()
        hand_copy(1, w).wait_send()


def solution(mesh):
    placed = (
        P(None, "chan", "wall", None),
        P("chan", "wall", None),
        P("chan", "wall", None),
        P("chan", "wall", None, None, None),
    )
    chan_count = mesh.shape["chan"]
    wall_count = mesh.shape["wall"]

    def on_device(coords, masses, counts, lists):
        vmem = pl.BlockSpec(memory_space=pltpu.VMEM)
        hbm = pl.BlockSpec(memory_space=pl.ANY)
        dma = pltpu.SemaphoreType.DMA
        density = pl.pallas_call(
            functools.partial(kernel, chan_count, wall_count),
            out_shape=jax.ShapeDtypeStruct((ROWS, 128), F32),
            in_specs=[hbm, hbm, hbm, hbm],
            out_specs=vmem,
            scratch_shapes=[
                pltpu.VMEM((3 * ROWS, 128), F32),
                pltpu.VMEM((ROWS, 128), F32),
                pltpu.SMEM((TILES,), jnp.int32),
                dma((5,)),
                pltpu.VMEM((2, 128, 128), F32),
                pltpu.VMEM((R + 1, 128, 128), F32),
                pltpu.VMEM((R + 1, R + 1, 2, 16), jnp.int32),
                pltpu.SMEM((R + 1, 2, 16), jnp.int32),
                pltpu.VMEM((2, TILES, 32, 128), F32),
                pltpu.VMEM((48, 32, 512), BF16),
                pltpu.VMEM((48, 16, TILE), F32),
                pltpu.VMEM((4 * TILE, 128), BF16),
                pltpu.VMEM((4 * TILE, 128), BF16),
                pltpu.VMEM((TILE, 512), F32),
                pltpu.VMEM((TILE, 512), F32),
                pltpu.VMEM((TILE, 128), F32),
                pltpu.VMEM((TILE, 128), F32),
                pltpu.VMEM((TILE, 128), F32),
                pltpu.VMEM((TILE, 128), F32),
                pltpu.VMEM((R + 1, ROWS, 128), F32),
                pltpu.VMEM((R, ROWS, 128), F32),
                pltpu.VMEM((32 * R, TILE), F32),
                pltpu.VMEM((1, 128), jnp.int32),
                pltpu.VMEM((96, 128), F32),
                pltpu.VMEM((2, ROWS, 128), F32),
                dma((R,)),
                dma((R,)),
                dma((2,)),
                dma((2,)),
                dma((R,)),
                dma((R,)),
                dma((R,)),
                dma((R,)),
                dma((2,)),
                dma((2,)),
                dma((R + 1,)),
            ],
            compiler_params=pltpu.CompilerParams(
                collective_id=0,
                has_side_effects=True,
            ),
        )(
            coords.reshape(3 * ROWS, 128),
            masses.reshape(ROWS, 128),
            counts.reshape(TILES),
            jnp.transpose(lists.reshape(R + 1, TILES, 2), (0, 2, 1)),
        )
        return density.reshape(1, 1, -1)

    return jax.shard_map(
        on_device, mesh=mesh, in_specs=placed, out_specs=P("chan", "wall", None), check_vma=False
    )
```

```python
import functools
import math

import jax
import jax.numpy as jnp
from jax import lax
from jax.experimental import pallas as pl
from jax.experimental.pallas import tpu as pltpu
from jax.sharding import PartitionSpec as P

R = 4
TILES = 16
TILE = 256
ROWS = 32
EPS = 0.0001 / (R * R)
CHUNK = 32
SPLIT = 8
FAR = 16.0
F32 = jnp.float32
BF16 = jnp.bfloat16
MESH = pl.DeviceIdType.MESH


def split3(value):
    high = value.astype(BF16).astype(F32)
    rest = value - high
    mid = rest.astype(BF16).astype(F32)
    low = (rest - mid).astype(BF16).astype(F32)
    return high, mid, low


def spread4(value, row):
    swapped = jnp.where(row % 2 == 0, pltpu.roll(value, 7, 1), pltpu.roll(value, 1, 1))
    value = value + swapped
    swapped = jnp.where(row % 4 < 2, pltpu.roll(value, 6, 1), pltpu.roll(value, 2, 1))
    return value + swapped


def halves(first, upper, lower, row):
    upper_turned, lower_turned = pltpu.roll(upper, 4, 1), pltpu.roll(lower, 4, 1)
    top = row < 4
    if first == 0:
        return jnp.where(top, upper, lower_turned)
    return jnp.where(top, upper_turned, lower)


def rows_of(value):
    return lax.broadcasted_iota(jnp.int32, value.shape, 1)


def features_a(packed, shift):
    row = rows_of(packed)
    moved = packed - jnp.where(row % 4 == 0, shift, 0.0)
    coord = row % 4 < 3
    norm = spread4(jnp.where(coord, moved * moved, 0.0), row) + EPS
    high, mid, low = split3(jnp.where(coord, -2.0 * moved, norm))
    mass = split3(spread4(jnp.where(coord, 0.0, packed), row))
    blocks = []
    for half in range(2):
        wide = [halves(half, part, part, row) for part in mass]
        last = jnp.where(row == 3, wide[0], jnp.where(row == 4, wide[1], wide[2]))
        last = jnp.where(row < 3, 1.0, jnp.where(row < 6, last, 0.0))
        blocks.append(
            [
                halves(half, high, high, row),
                halves(half, mid, mid, row),
                halves(half, high, low, row),
                last,
            ]
        )
    return blocks


def features_b(packed, lift):
    row = rows_of(packed)
    coord = row % 4 < 3
    mass = spread4(jnp.where(coord, 0.0, packed), row)
    empty = mass <= 0.0
    mass = jnp.where(empty, 1.0, mass)
    root = jnp.exp(jnp.log(mass) * (1.0 / 3.0))
    root = root - (root * root * root - mass) / (3.0 * root * root)
    square = root * root
    moved = packed + jnp.where(row % 4 == 1, lift, 0.0)
    moved = jnp.where(jnp.logical_and(row % 4 == 2, empty), FAR, moved)
    norm = spread4(jnp.where(coord, moved * moved, 0.0), row) * square
    moved = jnp.where(coord, moved, 1.0) * square
    blocks = []
    parts = []
    for factor in (1.0, 3.0):
        parts.append((split3(factor * moved), split3(factor * norm)))
    for half in range(2):
        block = []
        for (high, mid, low), last in parts:
            last = jnp.where(row % 4 == 0, last[0], jnp.where(row % 4 == 1, last[1], last[2]))
            last = jnp.where(row < 3, halves(half, last, last, row), 0.0)
            mixed = halves(half, high, mid, row)
            block.append([mixed, mixed, halves(half, low, high, row), last])
        block.append(halves(half, 2.0 * root, 2.0 * root, row))
        block.append(halves(half, 4.0 * mass, 4.0 * mass, row))
        blocks.append(block)
    return blocks


def kernel(
    chan_count,
    wall_count,
    coords_hbm,
    mass_hbm,
    counts_hbm,
    lists_hbm,
    out_ref,
    coords_ref,
    mass_ref,
    counts_ref,
    input_sem,
    walls,
    slabs,
    list_v,
    list_s,
    stage,
    feat_b,
    root_b,
    feat_a,
    feat_own,
    dots0,
    dots1,
    mass0,
    mass1,
    part_g,
    full_g,
    gained,
    gained_in,
    handed_rows,
    list_row,
    handed,
    handed_in,
    slab_send,
    slab_recv,
    wall_send,
    wall_recv,
    list_send,
    list_recv,
    gain_send,
    gain_recv,
    hand_send,
    hand_recv,
    list_copy,
):
    c = lax.axis_index("chan")
    w = lax.axis_index("wall")
    has_low = w > 0
    has_high = w < wall_count - 1

    def up(k):
        return (lax.rem(c + k, chan_count), w)

    def down(k):
        return (lax.rem(c + chan_count - k, chan_count), w)

    first = lax.rem(c, 2) == 0
    partner = (c + 1 - 2 * lax.rem(c, 2), w)
    barrier = pltpu.get_barrier_semaphore()
    pl.semaphore_signal(barrier, inc=1, device_id=down(2), device_id_type=MESH)
    pl.semaphore_signal(barrier, inc=1, device_id=partner, device_id_type=MESH)

    @pl.when(has_low)
    def _():
        pl.semaphore_signal(barrier, inc=1, device_id=(c, w - 1), device_id_type=MESH)

    @pl.when(has_high)
    def _():
        pl.semaphore_signal(barrier, inc=1, device_id=(c, w + 1), device_id_type=MESH)

    inputs = [
        pltpu.make_async_copy(source, target, input_sem.at[at])
        for at, (source, target) in enumerate(
            (
                (counts_hbm, counts_ref),
                (coords_hbm, coords_ref),
                (mass_hbm, mass_ref),
                (lists_hbm, list_v.at[R]),
                (lists_hbm.at[0], list_s.at[0]),
            )
        )
    ]
    for copy in inputs:
        copy.start()
    row_at = lax.broadcasted_iota(jnp.int32, (ROWS, 128), 0)
    lane_at = lax.broadcasted_iota(jnp.int32, (ROWS, 128), 1)
    slot_at = lax.rem(row_at, 2) * 128 + lane_at
    limit = jnp.zeros((ROWS, 128), jnp.int32)
    for copy in inputs:
        copy.wait()
    for t in range(TILES):
        limit = jnp.where(row_at // 2 == t, counts_ref[t], limit)
    filled = (slot_at < limit).astype(F32)
    own = slabs.at[R]
    own[pl.ds(0, ROWS, stride=4), :] = coords_ref[0:32, :] * (1.0 / R)
    own[pl.ds(1, ROWS, stride=4), :] = (coords_ref[32:64, :] - R) * (1.0 / R)
    own[pl.ds(2, ROWS, stride=4), :] = (coords_ref[64:96, :] - R) * (1.0 / R)
    own[pl.ds(3, ROWS, stride=4), :] = mass_ref[...] * filled
    list_row[...] = jnp.zeros_like(list_row)

    pl.semaphore_wait(barrier, 2 + has_low.astype(jnp.int32) + has_high.astype(jnp.int32))

    def wall_copy(slot, target):
        return pltpu.make_async_remote_copy(
            src_ref=own,
            dst_ref=walls.at[slot],
            send_sem=wall_send.at[slot],
            recv_sem=wall_recv.at[slot],
            device_id=(c, target),
            device_id_type=MESH,
        )

    def pass_on(source, k, target):
        slab = pltpu.make_async_remote_copy(
            src_ref=slabs.at[source],
            dst_ref=slabs.at[k - 1],
            send_sem=slab_send.at[k - 1],
            recv_sem=slab_recv.at[k - 1],
            device_id=target,
            device_id_type=MESH,
        )
        rows = pltpu.make_async_remote_copy(
            src_ref=list_v.at[source],
            dst_ref=list_v.at[k - 1],
            send_sem=list_send.at[k - 1],
            recv_sem=list_recv.at[k - 1],
            device_id=target,
            device_id_type=MESH,
        )
        return slab, rows

    def send(source, k, target):
        slab, rows = pass_on(source, k, target)
        rows.start()
        slab.start()

    def gain_copy(k):
        return pltpu.make_async_remote_copy(
            src_ref=gained.at[k],
            dst_ref=gained_in.at[k - 1],
            send_sem=gain_send.at[k - 1],
            recv_sem=gain_recv.at[k - 1],
            device_id=down(k),
            device_id_type=MESH,
        )

    def hand_copy(slot, target):
        return pltpu.make_async_remote_copy(
            src_ref=handed.at[pl.ds(64 * (1 - slot), ROWS)],
            dst_ref=handed_in.at[slot],
            send_sem=hand_send.at[slot],
            recv_sem=hand_recv.at[slot],
            device_id=(c, target),
            device_id_type=MESH,
        )

    crossing = c >= chan_count - 2

    @pl.when(crossing)
    def _():
        send(R, 2, up(2))

    @pl.when(has_high)
    def _():
        wall_copy(0, w + 1).start()

    @pl.when(has_low)
    def _():
        wall_copy(1, w - 1).start()

    @pl.when(jnp.logical_not(crossing))
    def _():
        send(R, 2, up(2))

    @pl.when(first)
    def _():
        send(R, 1, partner)

    def list_down(k):
        return pltpu.make_async_copy(list_v.at[k - 1, k], list_s.at[k], list_copy.at[k])

    def build_b(packed, side):
        blocks = features_b(packed.reshape(TILES, 8, 128), 2.0 * (side - 1))
        tiles = slice(side * TILES, side * TILES + TILES)
        for half, (plain, triple, root, mass) in enumerate(blocks):
            lanes = slice(half * 128, half * 128 + 128)
            for at, rows in ((0, plain), (256, triple)):
                wide = slice(at + half * 128, at + half * 128 + 128)
                for g in range(0, 4, 2):
                    both = jnp.concatenate(rows[g : g + 2], axis=1).astype(BF16)
                    feat_b[tiles, 8 * g : 8 * g + 16, wide] = both
            root_b[tiles, 0:8, lanes] = root
            root_b[tiles, 8:16, lanes] = mass

    def build_a(feat, packed, shift):
        blocks = features_a(packed.reshape(TILES, 8, 128), shift)
        for half in range(2):
            for g in range(4):
                stage[half, :, 8 * g : 8 * g + 8, :] = blocks[half][g]
        for q in range(TILES // 4):
            for half in range(2):
                spot = q * TILE + half * 128
                turned = stage[half, 4 * q : 4 * q + 4].reshape(128, 128).T
                feat[spot : spot + 128, :] = turned.astype(BF16)

    build_a(feat_own, own[...], 0.0)
    build_b(own[...], 1)

    @pl.when(has_low)
    def _():
        wall_copy(0, w).wait_recv()

    @pl.when(jnp.logical_not(has_low))
    def _():
        walls[0] = jnp.zeros_like(walls[0])

    build_b(walls[0], 0)

    @pl.when(has_high)
    def _():
        wall_copy(1, w).wait_recv()

    @pl.when(jnp.logical_not(has_high))
    def _():
        walls[1] = jnp.zeros_like(walls[1])

    build_b(walls[1], 2)

    lane_row = lax.broadcasted_iota(jnp.int32, (1, 128), 1)
    pick_at = lax.broadcasted_iota(jnp.int32, (32, 128), 0)
    pick = jnp.logical_and(pick_at >= 27, pick_at < 30).astype(F32).astype(BF16)

    def placed(rows, quarter):
        width = rows.shape[1]
        parts = [jnp.zeros((32 * quarter, width), BF16)] if quarter else []
        parts.append(rows)
        if quarter < 3:
            parts.append(jnp.zeros((96 - 32 * quarter, width), BF16))
        return jnp.concatenate(parts, axis=0)


    def pair(dots, roots, mass, source, target):
        taken = jnp.zeros((8, TILE), F32)
        root = roots[0:8, :][None]
        top = roots[8:16, :][None]
        for r in range(0, TILE, CHUNK):
            square = dots[r : r + CHUNK, 0:TILE].reshape(CHUNK // 8, 8, TILE)
            triple = dots[r : r + CHUNK, TILE : 2 * TILE].reshape(CHUNK // 8, 8, TILE)
            near = root - square * lax.rsqrt(square)
            outer = near * near * near
            inner = top - triple * near
            value = lax.clamp(jnp.zeros_like(inner), outer, inner)
            low, high = value[:, :, 0:128], value[:, :, 128:256]
            row = (low + high).reshape(CHUNK, 128)
            if source is not None:
                row = row + source[r : r + CHUNK, :]
            target[r : r + CHUNK, :] = row
            weight = mass[r : r + CHUNK, :].reshape(CHUNK // 8, 8, 128)
            back = jnp.concatenate([low * weight, high * weight], axis=2)
            for e in range(CHUNK // 8):
                taken = taken + back[e]
        return jnp.sum(taken, axis=0, keepdims=True)

    def section(step, k, feat, begin, end):
        def a_tile(i):
            return feat[(i // 4) * TILE : (i // 4) * TILE + TILE, :]

        def dot_into(dots, i, n):
            rows = placed(feat_b[list_s[k, n, i]], i % 4)
            dots[...] = jnp.dot(a_tile(i), rows, preferred_element_type=F32)

        def mass_into(mass, i):
            mass[...] = jnp.dot(a_tile(i), placed(pick, i % 4), preferred_element_type=F32)

        def flush(i):
            summed = jnp.sum(full_g[...].T, axis=0, keepdims=True)
            gained[k, 2 * i : 2 * i + 1, :] = summed[:, 0:128]
            gained[k, 2 * i + 1 : 2 * i + 2, :] = summed[:, 128:256]

        def note(i, n, row):
            if step is not None:
                at = step * 32 + 2 * i + n
                handed_rows[pl.ds(at, 1), :] = row
                list_row[...] = jnp.where(lane_row == at, list_s[k, n, i], list_row[...])

        masses = (mass0, mass1)
        dot_into(dots0, begin, 0)
        mass_into(mass0, begin)
        for i in range(begin, end):
            mass = masses[(i - begin) % 2]
            dot_into(dots1, i, 1)
            if i > begin:
                flush(i - 1)
            note(i, 0, pair(dots0, root_b.at[list_s[k, 0, i]], mass, None, part_g))
            if i + 1 < end:
                dot_into(dots0, i + 1, 0)
                mass_into(masses[(i + 1 - begin) % 2], i + 1)
            note(i, 1, pair(dots1, root_b.at[list_s[k, 1, i]], mass, part_g, full_g))
        flush(end - 1)

    late = c < 2

    def take(k):
        slab, rows = pass_on(R, k, partner)
        rows.wait_recv()
        slab.wait_recv()

    def relay():
        take(2)
        send(1, 4, up(2))

        @pl.when(first)
        def _():
            send(1, 3, partner)

        @pl.when(jnp.logical_not(first))
        def _():
            send(1, 1, partner)

    pl.when(jnp.logical_not(late))(relay)
    section(None, 0, feat_own, 0, SPLIT)
    pl.when(late)(relay)

    def one_offset(step, carry):
        k = jnp.where(step < 2, 2 - step, 6 - step)

        @pl.when(step > 0)
        def _():
            take(k)

        list_down(k).start()

        @pl.when(jnp.logical_and(step == 2, jnp.logical_not(first)))
        def _():
            send(3, 3, partner)

        build_a(feat_a, slabs[k - 1], k.astype(F32) * (1.0 / R))
        list_down(k).wait()
        section(step, k, feat_a, 0, TILES)
        gain_copy(k).start()
        return carry

    lax.fori_loop(0, R, one_offset, 0)

    known = list_row[...]
    hot = (lax.broadcasted_iota(jnp.int32, (48, 128), 0) == known).astype(F32).astype(BF16)
    summed = jnp.zeros((48, TILE), F32)
    for piece in split3(handed_rows[...]):
        summed = summed + jnp.dot(hot, piece.astype(BF16), preferred_element_type=F32)
    handed[pl.ds(0, 48, stride=2), :] = summed[:, 0:128]
    handed[pl.ds(1, 48, stride=2), :] = summed[:, 128:256]

    @pl.when(has_high)
    def _():
        hand_copy(0, w + 1).start()

    @pl.when(has_low)
    def _():
        hand_copy(1, w - 1).start()

    section(None, 0, feat_own, SPLIT, TILES)

    total = gained[0]
    for k in range(1, R + 1):
        gain_copy(k).wait_recv()
        total = total + gained_in[k - 1]
    out_ref[...] = handed[32:64, :]

    @pl.when(has_low)
    def _():
        hand_copy(0, w).wait_recv()
        out_ref[...] += handed_in[0]

    @pl.when(has_high)
    def _():
        hand_copy(1, w).wait_recv()
        out_ref[...] += handed_in[1]

    scale = filled * (1.0 / (4.0 * math.pi * 2 * TILE))
    out_ref[...] = (total + out_ref[...] / mass_ref[...]) * scale

    for k in range(1, R + 1):
        slab, rows = pass_on(R, k, partner)
        slab.wait_send()
        rows.wait_send()
        gain_copy(k).wait_send()

    @pl.when(has_high)
    def _():
        wall_copy(0, w).wait_send()
        hand_copy(0, w).wait_send()

    @pl.when(has_low)
    def _():
        wall_copy(1, w).wait_send()
        hand_copy(1, w).wait_send()


def solution(mesh):
    placed = (
        P(None, "chan", "wall", None),
        P("chan", "wall", None),
        P("chan", "wall", None),
        P("chan", "wall", None, None, None),
    )
    chan_count = mesh.shape["chan"]
    wall_count = mesh.shape["wall"]

    def on_device(coords, masses, counts, lists):
        vmem = pl.BlockSpec(memory_space=pltpu.VMEM)
        hbm = pl.BlockSpec(memory_space=pl.ANY)
        dma = pltpu.SemaphoreType.DMA
        density = pl.pallas_call(
            functools.partial(kernel, chan_count, wall_count),
            out_shape=pltpu.VMEM((ROWS, 128), F32),
            in_specs=[hbm, hbm, hbm, hbm],
            out_specs=vmem,
            scratch_shapes=[
                pltpu.VMEM((3 * ROWS, 128), F32),
                pltpu.VMEM((ROWS, 128), F32),
                pltpu.SMEM((TILES,), jnp.int32),
                dma((5,)),
                pltpu.VMEM((2, 128, 128), F32),
                pltpu.VMEM((R + 1, 128, 128), F32),
                pltpu.VMEM((R + 1, R + 1, 2, 16), jnp.int32),
                pltpu.SMEM((R + 1, 2, 16), jnp.int32),
                pltpu.VMEM((2, TILES, 32, 128), F32),
                pltpu.VMEM((48, 32, 512), BF16),
                pltpu.VMEM((48, 16, TILE), F32),
                pltpu.VMEM((4 * TILE, 128), BF16),
                pltpu.VMEM((4 * TILE, 128), BF16),
                pltpu.VMEM((TILE, 512), F32),
                pltpu.VMEM((TILE, 512), F32),
                pltpu.VMEM((TILE, 128), F32),
                pltpu.VMEM((TILE, 128), F32),
                pltpu.VMEM((TILE, 128), F32),
                pltpu.VMEM((TILE, 128), F32),
                pltpu.VMEM((R + 1, ROWS, 128), F32),
                pltpu.VMEM((R, ROWS, 128), F32),
                pltpu.VMEM((32 * R, TILE), F32),
                pltpu.VMEM((1, 128), jnp.int32),
                pltpu.VMEM((96, 128), F32),
                pltpu.VMEM((2, ROWS, 128), F32),
                dma((R,)),
                dma((R,)),
                dma((2,)),
                dma((2,)),
                dma((R,)),
                dma((R,)),
                dma((R,)),
                dma((R,)),
                dma((2,)),
                dma((2,)),
                dma((R + 1,)),
            ],
            compiler_params=pltpu.CompilerParams(
                collective_id=0,
                has_side_effects=True,
            ),
        )(
            coords.reshape(3 * ROWS, 128),
            masses.reshape(ROWS, 128),
            counts.reshape(TILES),
            jnp.transpose(lists.reshape(R + 1, TILES, 2), (0, 2, 1)),
        )
        return density.reshape(1, 1, -1)

    return jax.shard_map(
        on_device, mesh=mesh, in_specs=placed, out_specs=P("chan", "wall", None), check_vma=False
    )
```

```python
import functools
import math

import jax
import jax.numpy as jnp
from jax import lax
from jax.experimental import pallas as pl
from jax.experimental.pallas import tpu as pltpu
from jax.sharding import PartitionSpec as P

R = 4
TILES = 16
TILE = 256
ROWS = 32
EPS = 0.0001 / (R * R)
CHUNK = 32
SPLIT = 4
FAR = 16.0
F32 = jnp.float32
BF16 = jnp.bfloat16
MESH = pl.DeviceIdType.MESH


def split3(value):
    high = value.astype(BF16).astype(F32)
    rest = value - high
    mid = rest.astype(BF16).astype(F32)
    low = (rest - mid).astype(BF16).astype(F32)
    return high, mid, low


def spread4(value, row):
    swapped = jnp.where(row % 2 == 0, pltpu.roll(value, 7, 1), pltpu.roll(value, 1, 1))
    value = value + swapped
    swapped = jnp.where(row % 4 < 2, pltpu.roll(value, 6, 1), pltpu.roll(value, 2, 1))
    return value + swapped


def halves(first, upper, lower, row):
    upper_turned, lower_turned = pltpu.roll(upper, 4, 1), pltpu.roll(lower, 4, 1)
    top = row < 4
    if first == 0:
        return jnp.where(top, upper, lower_turned)
    return jnp.where(top, upper_turned, lower)


def rows_of(value):
    return lax.broadcasted_iota(jnp.int32, value.shape, 1)


def features_a(packed, shift):
    row = rows_of(packed)
    moved = packed - jnp.where(row % 4 == 0, shift, 0.0)
    coord = row % 4 < 3
    norm = spread4(jnp.where(coord, moved * moved, 0.0), row) + EPS
    high, mid, low = split3(jnp.where(coord, -2.0 * moved, norm))
    mass = split3(spread4(jnp.where(coord, 0.0, packed), row))
    blocks = []
    for half in range(2):
        wide = [halves(half, part, part, row) for part in mass]
        last = jnp.where(row == 3, wide[0], jnp.where(row == 4, wide[1], wide[2]))
        last = jnp.where(row < 3, 1.0, jnp.where(row < 6, last, 0.0))
        blocks.append(
            [
                halves(half, high, high, row),
                halves(half, mid, mid, row),
                halves(half, high, low, row),
                last,
            ]
        )
    return blocks


def features_b(packed, lift):
    row = rows_of(packed)
    coord = row % 4 < 3
    mass = spread4(jnp.where(coord, 0.0, packed), row)
    empty = mass <= 0.0
    mass = jnp.where(empty, 1.0, mass)
    root = jnp.exp(jnp.log(mass) * (1.0 / 3.0))
    root = root - (root * root * root - mass) / (3.0 * root * root)
    square = root * root
    moved = packed + jnp.where(row % 4 == 1, lift, 0.0)
    moved = jnp.where(jnp.logical_and(row % 4 == 2, empty), FAR, moved)
    norm = spread4(jnp.where(coord, moved * moved, 0.0), row) * square
    moved = jnp.where(coord, moved, 1.0) * square
    blocks = []
    parts = []
    for factor in (1.0, 3.0):
        parts.append((split3(factor * moved), split3(factor * norm)))
    for half in range(2):
        block = []
        for (high, mid, low), last in parts:
            last = jnp.where(row % 4 == 0, last[0], jnp.where(row % 4 == 1, last[1], last[2]))
            last = jnp.where(row < 3, halves(half, last, last, row), 0.0)
            mixed = halves(half, high, mid, row)
            block.append([mixed, mixed, halves(half, low, high, row), last])
        block.append(halves(half, 2.0 * root, 2.0 * root, row))
        block.append(halves(half, 4.0 * mass, 4.0 * mass, row))
        blocks.append(block)
    return blocks


def kernel(
    chan_count,
    wall_count,
    coords_hbm,
    mass_hbm,
    counts_hbm,
    lists_hbm,
    out_ref,
    coords_ref,
    mass_ref,
    counts_ref,
    input_sem,
    walls,
    slabs,
    list_v,
    list_s,
    stage,
    feat_b,
    root_b,
    feat_a,
    feat_own,
    dots0,
    dots1,
    mass0,
    mass1,
    part_g,
    full_g,
    gained,
    gained_in,
    handed_rows,
    list_row,
    handed,
    handed_in,
    slab_send,
    slab_recv,
    wall_send,
    wall_recv,
    list_send,
    list_recv,
    gain_send,
    gain_recv,
    hand_send,
    hand_recv,
    list_copy,
):
    c = lax.axis_index("chan")
    w = lax.axis_index("wall")
    has_low = w > 0
    has_high = w < wall_count - 1

    def up(k):
        return (lax.rem(c + k, chan_count), w)

    def down(k):
        return (lax.rem(c + chan_count - k, chan_count), w)

    first = lax.rem(c, 2) == 0
    partner = (c + 1 - 2 * lax.rem(c, 2), w)
    barrier = pltpu.get_barrier_semaphore()
    pl.semaphore_signal(barrier, inc=1, device_id=down(2), device_id_type=MESH)
    pl.semaphore_signal(barrier, inc=1, device_id=partner, device_id_type=MESH)

    @pl.when(has_low)
    def _():
        pl.semaphore_signal(barrier, inc=1, device_id=(c, w - 1), device_id_type=MESH)

    @pl.when(has_high)
    def _():
        pl.semaphore_signal(barrier, inc=1, device_id=(c, w + 1), device_id_type=MESH)

    inputs = [
        pltpu.make_async_copy(source, target, input_sem.at[at])
        for at, (source, target) in enumerate(
            (
                (counts_hbm, counts_ref),
                (coords_hbm, coords_ref),
                (mass_hbm, mass_ref),
                (lists_hbm, list_v.at[R]),
                (lists_hbm.at[0], list_s.at[0]),
            )
        )
    ]
    for copy in inputs:
        copy.start()
    row_at = lax.broadcasted_iota(jnp.int32, (ROWS, 128), 0)
    lane_at = lax.broadcasted_iota(jnp.int32, (ROWS, 128), 1)
    slot_at = lax.rem(row_at, 2) * 128 + lane_at
    limit = jnp.zeros((ROWS, 128), jnp.int32)
    for copy in inputs:
        copy.wait()
    for t in range(TILES):
        limit = jnp.where(row_at // 2 == t, counts_ref[t], limit)
    filled = (slot_at < limit).astype(F32)
    own = slabs.at[R]
    own[pl.ds(0, ROWS, stride=4), :] = coords_ref[0:32, :] * (1.0 / R)
    own[pl.ds(1, ROWS, stride=4), :] = (coords_ref[32:64, :] - R) * (1.0 / R)
    own[pl.ds(2, ROWS, stride=4), :] = (coords_ref[64:96, :] - R) * (1.0 / R)
    own[pl.ds(3, ROWS, stride=4), :] = mass_ref[...] * filled
    list_row[...] = jnp.zeros_like(list_row)

    pl.semaphore_wait(barrier, 2 + has_low.astype(jnp.int32) + has_high.astype(jnp.int32))

    def wall_copy(slot, target):
        return pltpu.make_async_remote_copy(
            src_ref=own,
            dst_ref=walls.at[slot],
            send_sem=wall_send.at[slot],
            recv_sem=wall_recv.at[slot],
            device_id=(c, target),
            device_id_type=MESH,
        )

    def pass_on(source, k, target):
        slab = pltpu.make_async_remote_copy(
            src_ref=slabs.at[source],
            dst_ref=slabs.at[k - 1],
            send_sem=slab_send.at[k - 1],
            recv_sem=slab_recv.at[k - 1],
            device_id=target,
            device_id_type=MESH,
        )
        rows = pltpu.make_async_remote_copy(
            src_ref=list_v.at[source],
            dst_ref=list_v.at[k - 1],
            send_sem=list_send.at[k - 1],
            recv_sem=list_recv.at[k - 1],
            device_id=target,
            device_id_type=MESH,
        )
        return slab, rows

    def send(source, k, target):
        slab, rows = pass_on(source, k, target)
        rows.start()
        slab.start()

    def gain_copy(k):
        return pltpu.make_async_remote_copy(
            src_ref=gained.at[k],
            dst_ref=gained_in.at[k - 1],
            send_sem=gain_send.at[k - 1],
            recv_sem=gain_recv.at[k - 1],
            device_id=down(k),
            device_id_type=MESH,
        )

    def hand_copy(slot, target):
        return pltpu.make_async_remote_copy(
            src_ref=handed.at[pl.ds(64 * (1 - slot), ROWS)],
            dst_ref=handed_in.at[slot],
            send_sem=hand_send.at[slot],
            recv_sem=hand_recv.at[slot],
            device_id=(c, target),
            device_id_type=MESH,
        )

    crossing = c == chan_count - 2
    yielding = c == chan_count - 1

    @pl.when(crossing)
    def _():
        send(R, 2, up(2))

    @pl.when(has_high)
    def _():
        wall_copy(0, w + 1).start()

    @pl.when(has_low)
    def _():
        wall_copy(1, w - 1).start()

    @pl.when(c < chan_count - 2)
    def _():
        send(R, 2, up(2))

    @pl.when(first)
    def _():
        send(R, 1, partner)

    def list_down(k):
        return pltpu.make_async_copy(list_v.at[k - 1, k], list_s.at[k], list_copy.at[k])

    def build_b(packed, side):
        blocks = features_b(packed.reshape(TILES, 8, 128), 2.0 * (side - 1))
        tiles = slice(side * TILES, side * TILES + TILES)
        for half, (plain, triple, root, mass) in enumerate(blocks):
            lanes = slice(half * 128, half * 128 + 128)
            for at, rows in ((0, plain), (256, triple)):
                wide = slice(at + half * 128, at + half * 128 + 128)
                for g in range(0, 4, 2):
                    both = jnp.concatenate(rows[g : g + 2], axis=1).astype(BF16)
                    feat_b[tiles, 8 * g : 8 * g + 16, wide] = both
            root_b[tiles, 0:8, lanes] = root
            root_b[tiles, 8:16, lanes] = mass

    def build_a(feat, packed, shift):
        blocks = features_a(packed.reshape(TILES, 8, 128), shift)
        for half in range(2):
            for g in range(4):
                stage[half, :, 8 * g : 8 * g + 8, :] = blocks[half][g]
        for q in range(TILES // 4):
            for half in range(2):
                spot = q * TILE + half * 128
                turned = stage[half, 4 * q : 4 * q + 4].reshape(128, 128).T
                feat[spot : spot + 128, :] = turned.astype(BF16)

    build_a(feat_own, own[...], 0.0)
    build_b(own[...], 1)

    @pl.when(yielding)
    def _():
        send(R, 2, up(2))

    @pl.when(has_low)
    def _():
        wall_copy(0, w).wait_recv()

    @pl.when(jnp.logical_not(has_low))
    def _():
        walls[0] = jnp.zeros_like(walls[0])

    build_b(walls[0], 0)

    @pl.when(has_high)
    def _():
        wall_copy(1, w).wait_recv()

    @pl.when(jnp.logical_not(has_high))
    def _():
        walls[1] = jnp.zeros_like(walls[1])

    build_b(walls[1], 2)

    lane_row = lax.broadcasted_iota(jnp.int32, (1, 128), 1)
    pick_at = lax.broadcasted_iota(jnp.int32, (32, 128), 0)
    pick = jnp.logical_and(pick_at >= 27, pick_at < 30).astype(F32).astype(BF16)

    def placed(rows, quarter):
        width = rows.shape[1]
        parts = [jnp.zeros((32 * quarter, width), BF16)] if quarter else []
        parts.append(rows)
        if quarter < 3:
            parts.append(jnp.zeros((96 - 32 * quarter, width), BF16))
        return jnp.concatenate(parts, axis=0)


    def pair(dots, roots, mass, source, target):
        taken = jnp.zeros((8, TILE), F32)
        root = roots[0:8, :][None]
        top = roots[8:16, :][None]
        for r in range(0, TILE, CHUNK):
            square = dots[r : r + CHUNK, 0:TILE].reshape(CHUNK // 8, 8, TILE)
            triple = dots[r : r + CHUNK, TILE : 2 * TILE].reshape(CHUNK // 8, 8, TILE)
            near = root - square * lax.rsqrt(square)
            outer = near * near * near
            inner = top - triple * near
            value = lax.clamp(jnp.zeros_like(inner), outer, inner)
            low, high = value[:, :, 0:128], value[:, :, 128:256]
            row = (low + high).reshape(CHUNK, 128)
            if source is not None:
                row = row + source[r : r + CHUNK, :]
            target[r : r + CHUNK, :] = row
            weight = mass[r : r + CHUNK, :].reshape(CHUNK // 8, 8, 128)
            back = jnp.concatenate([low * weight, high * weight], axis=2)
            for e in range(CHUNK // 8):
                taken = taken + back[e]
        return jnp.sum(taken, axis=0, keepdims=True)

    def section(step, k, feat, begin, end):
        def a_tile(i):
            return feat[(i // 4) * TILE : (i // 4) * TILE + TILE, :]

        def dot_into(dots, i, n):
            rows = placed(feat_b[list_s[k, n, i]], i % 4)
            dots[...] = jnp.dot(a_tile(i), rows, preferred_element_type=F32)

        def mass_into(mass, i):
            mass[...] = jnp.dot(a_tile(i), placed(pick, i % 4), preferred_element_type=F32)

        def flush(i):
            summed = jnp.sum(full_g[...].T, axis=0, keepdims=True)
            gained[k, 2 * i : 2 * i + 1, :] = summed[:, 0:128]
            gained[k, 2 * i + 1 : 2 * i + 2, :] = summed[:, 128:256]

        def note(i, n, row):
            if step is not None:
                at = step * 32 + 2 * i + n
                handed_rows[pl.ds(at, 1), :] = row
                list_row[...] = jnp.where(lane_row == at, list_s[k, n, i], list_row[...])

        masses = (mass0, mass1)
        dot_into(dots0, begin, 0)
        mass_into(mass0, begin)
        for i in range(begin, end):
            mass = masses[(i - begin) % 2]
            dot_into(dots1, i, 1)
            if i > begin:
                flush(i - 1)
            note(i, 0, pair(dots0, root_b.at[list_s[k, 0, i]], mass, None, part_g))
            if i + 1 < end:
                dot_into(dots0, i + 1, 0)
                mass_into(masses[(i + 1 - begin) % 2], i + 1)
            note(i, 1, pair(dots1, root_b.at[list_s[k, 1, i]], mass, part_g, full_g))
        flush(end - 1)

    late = c < 2

    def take(k):
        slab, rows = pass_on(R, k, partner)
        rows.wait_recv()
        slab.wait_recv()

    def relay():
        take(2)
        send(1, 4, up(2))

        @pl.when(first)
        def _():
            send(1, 3, partner)

        @pl.when(jnp.logical_not(first))
        def _():
            send(1, 1, partner)

    pl.when(jnp.logical_not(late))(relay)
    section(None, 0, feat_own, 0, SPLIT)
    pl.when(jnp.logical_and(late, first))(relay)

    def one_offset(step, carry):
        near = jnp.where(first, 2 - step, 1 + step)
        k = jnp.where(step < 2, near, 6 - step)
        pl.when(jnp.logical_and(step == 1, jnp.logical_and(late, jnp.logical_not(first))))(relay)

        @pl.when(k != 2)
        def _():
            take(k)

        list_down(k).start()

        @pl.when(jnp.logical_and(step == 2, jnp.logical_not(first)))
        def _():
            send(3, 3, partner)

        build_a(feat_a, slabs[k - 1], k.astype(F32) * (1.0 / R))
        list_down(k).wait()
        section(step, k, feat_a, 0, TILES)
        gain_copy(k).start()
        return carry

    lax.fori_loop(0, R, one_offset, 0)

    known = list_row[...]
    hot = (lax.broadcasted_iota(jnp.int32, (48, 128), 0) == known).astype(F32).astype(BF16)
    summed = jnp.zeros((48, TILE), F32)
    for piece in split3(handed_rows[...]):
        summed = summed + jnp.dot(hot, piece.astype(BF16), preferred_element_type=F32)
    handed[pl.ds(0, 48, stride=2), :] = summed[:, 0:128]
    handed[pl.ds(1, 48, stride=2), :] = summed[:, 128:256]

    @pl.when(has_high)
    def _():
        hand_copy(0, w + 1).start()

    @pl.when(has_low)
    def _():
        hand_copy(1, w - 1).start()

    section(None, 0, feat_own, SPLIT, TILES)

    total = gained[0]
    for k in range(1, R + 1):
        gain_copy(k).wait_recv()
        total = total + gained_in[k - 1]
    out_ref[...] = handed[32:64, :]

    @pl.when(has_low)
    def _():
        hand_copy(0, w).wait_recv()
        out_ref[...] += handed_in[0]

    @pl.when(has_high)
    def _():
        hand_copy(1, w).wait_recv()
        out_ref[...] += handed_in[1]

    scale = filled * (1.0 / (4.0 * math.pi * 2 * TILE))
    out_ref[...] = (total + out_ref[...] / mass_ref[...]) * scale

    for k in range(1, R + 1):
        slab, rows = pass_on(R, k, partner)
        slab.wait_send()
        rows.wait_send()
        gain_copy(k).wait_send()

    @pl.when(has_high)
    def _():
        wall_copy(0, w).wait_send()
        hand_copy(0, w).wait_send()

    @pl.when(has_low)
    def _():
        wall_copy(1, w).wait_send()
        hand_copy(1, w).wait_send()


def solution(mesh):
    placed = (
        P(None, "chan", "wall", None),
        P("chan", "wall", None),
        P("chan", "wall", None),
        P("chan", "wall", None, None, None),
    )
    chan_count = mesh.shape["chan"]
    wall_count = mesh.shape["wall"]

    def on_device(coords, masses, counts, lists):
        vmem = pl.BlockSpec(memory_space=pltpu.VMEM)
        hbm = pl.BlockSpec(memory_space=pl.ANY)
        dma = pltpu.SemaphoreType.DMA
        density = pl.pallas_call(
            functools.partial(kernel, chan_count, wall_count),
            out_shape=pltpu.VMEM((ROWS, 128), F32),
            in_specs=[hbm, hbm, hbm, hbm],
            out_specs=vmem,
            scratch_shapes=[
                pltpu.VMEM((3 * ROWS, 128), F32),
                pltpu.VMEM((ROWS, 128), F32),
                pltpu.SMEM((TILES,), jnp.int32),
                dma((5,)),
                pltpu.VMEM((2, 128, 128), F32),
                pltpu.VMEM((R + 1, 128, 128), F32),
                pltpu.VMEM((R + 1, R + 1, 2, 16), jnp.int32),
                pltpu.SMEM((R + 1, 2, 16), jnp.int32),
                pltpu.VMEM((2, TILES, 32, 128), F32),
                pltpu.VMEM((48, 32, 512), BF16),
                pltpu.VMEM((48, 16, TILE), F32),
                pltpu.VMEM((4 * TILE, 128), BF16),
                pltpu.VMEM((4 * TILE, 128), BF16),
                pltpu.VMEM((TILE, 512), F32),
                pltpu.VMEM((TILE, 512), F32),
                pltpu.VMEM((TILE, 128), F32),
                pltpu.VMEM((TILE, 128), F32),
                pltpu.VMEM((TILE, 128), F32),
                pltpu.VMEM((TILE, 128), F32),
                pltpu.VMEM((R + 1, ROWS, 128), F32),
                pltpu.VMEM((R, ROWS, 128), F32),
                pltpu.VMEM((32 * R, TILE), F32),
                pltpu.VMEM((1, 128), jnp.int32),
                pltpu.VMEM((96, 128), F32),
                pltpu.VMEM((2, ROWS, 128), F32),
                dma((R,)),
                dma((R,)),
                dma((2,)),
                dma((2,)),
                dma((R,)),
                dma((R,)),
                dma((R,)),
                dma((R,)),
                dma((2,)),
                dma((2,)),
                dma((R + 1,)),
            ],
            compiler_params=pltpu.CompilerParams(
                collective_id=0,
                has_side_effects=True,
            ),
        )(
            coords.reshape(3 * ROWS, 128),
            masses.reshape(ROWS, 128),
            counts.reshape(TILES),
            jnp.transpose(lists.reshape(R + 1, TILES, 2), (0, 2, 1)),
        )
        return density.reshape(1, 1, -1)

    return jax.shard_map(
        on_device, mesh=mesh, in_specs=placed, out_specs=P("chan", "wall", None), check_vma=False
    )
```

```python
import functools
import math

import jax
import jax.numpy as jnp
from jax import lax
from jax.experimental import pallas as pl
from jax.experimental.pallas import tpu as pltpu
from jax.sharding import PartitionSpec as P

R = 4
TILES = 16
TILE = 256
ROWS = 32
EPS = 0.0001 / (R * R)
CHUNK = 32
SPLIT = 4
FAR = 16.0
F32 = jnp.float32
BF16 = jnp.bfloat16
MESH = pl.DeviceIdType.MESH


def split3(value):
    high = value.astype(BF16).astype(F32)
    rest = value - high
    mid = rest.astype(BF16).astype(F32)
    low = (rest - mid).astype(BF16).astype(F32)
    return high, mid, low


def spread4(value, row):
    swapped = jnp.where(row % 2 == 0, pltpu.roll(value, 7, 1), pltpu.roll(value, 1, 1))
    value = value + swapped
    swapped = jnp.where(row % 4 < 2, pltpu.roll(value, 6, 1), pltpu.roll(value, 2, 1))
    return value + swapped


def halves(first, upper, lower, row):
    upper_turned, lower_turned = pltpu.roll(upper, 4, 1), pltpu.roll(lower, 4, 1)
    top = row < 4
    if first == 0:
        return jnp.where(top, upper, lower_turned)
    return jnp.where(top, upper_turned, lower)


def rows_of(value):
    return lax.broadcasted_iota(jnp.int32, value.shape, 1)


def features_a(packed, shift):
    row = rows_of(packed)
    moved = packed - jnp.where(row % 4 == 0, shift, 0.0)
    coord = row % 4 < 3
    norm = spread4(jnp.where(coord, moved * moved, 0.0), row) + EPS
    high, mid, low = split3(jnp.where(coord, -2.0 * moved, norm))
    mass = split3(spread4(jnp.where(coord, 0.0, packed), row))
    blocks = []
    for half in range(2):
        wide = [halves(half, part, part, row) for part in mass]
        last = jnp.where(row == 3, wide[0], jnp.where(row == 4, wide[1], wide[2]))
        last = jnp.where(row < 3, 1.0, jnp.where(row < 6, last, 0.0))
        blocks.append(
            [
                halves(half, high, high, row),
                halves(half, mid, mid, row),
                halves(half, high, low, row),
                last,
            ]
        )
    return blocks


def features_b(packed, lift):
    row = rows_of(packed)
    coord = row % 4 < 3
    mass = spread4(jnp.where(coord, 0.0, packed), row)
    empty = mass <= 0.0
    mass = jnp.where(empty, 1.0, mass)
    root = jnp.exp(jnp.log(mass) * (1.0 / 3.0))
    root = root - (root * root * root - mass) / (3.0 * root * root)
    square = root * root
    moved = packed + jnp.where(row % 4 == 1, lift, 0.0)
    moved = jnp.where(jnp.logical_and(row % 4 == 2, empty), FAR, moved)
    norm = spread4(jnp.where(coord, moved * moved, 0.0), row) * square
    moved = jnp.where(coord, moved, 1.0) * square
    blocks = []
    parts = []
    for factor in (1.0, 3.0):
        parts.append((split3(factor * moved), split3(factor * norm)))
    for half in range(2):
        block = []
        for (high, mid, low), last in parts:
            last = jnp.where(row % 4 == 0, last[0], jnp.where(row % 4 == 1, last[1], last[2]))
            last = jnp.where(row < 3, halves(half, last, last, row), 0.0)
            mixed = halves(half, high, mid, row)
            block.append([mixed, mixed, halves(half, low, high, row), last])
        block.append(halves(half, 2.0 * root, 2.0 * root, row))
        block.append(halves(half, 4.0 * mass, 4.0 * mass, row))
        blocks.append(block)
    return blocks


def kernel(
    chan_count,
    wall_count,
    coords_hbm,
    mass_hbm,
    counts_hbm,
    lists_hbm,
    out_ref,
    coords_ref,
    mass_ref,
    counts_ref,
    input_sem,
    walls,
    slabs,
    list_v,
    list_s,
    stage,
    feat_b,
    root_b,
    feat_a,
    feat_own,
    dots0,
    dots1,
    mass0,
    mass1,
    part_g,
    full_g,
    gained,
    gained_in,
    handed_rows,
    list_row,
    handed,
    handed_in,
    slab_send,
    slab_recv,
    wall_send,
    wall_recv,
    list_send,
    list_recv,
    gain_send,
    gain_recv,
    hand_send,
    hand_recv,
    list_copy,
):
    c = lax.axis_index("chan")
    w = lax.axis_index("wall")
    has_low = w > 0
    has_high = w < wall_count - 1

    def up(k):
        return (lax.rem(c + k, chan_count), w)

    def down(k):
        return (lax.rem(c + chan_count - k, chan_count), w)

    first = lax.rem(c, 2) == 0
    partner = (c + 1 - 2 * lax.rem(c, 2), w)
    barrier = pltpu.get_barrier_semaphore()
    pl.semaphore_signal(barrier, inc=1, device_id=down(2), device_id_type=MESH)
    pl.semaphore_signal(barrier, inc=1, device_id=partner, device_id_type=MESH)

    @pl.when(has_low)
    def _():
        pl.semaphore_signal(barrier, inc=1, device_id=(c, w - 1), device_id_type=MESH)

    @pl.when(has_high)
    def _():
        pl.semaphore_signal(barrier, inc=1, device_id=(c, w + 1), device_id_type=MESH)

    inputs = [
        pltpu.make_async_copy(source, target, input_sem.at[at])
        for at, (source, target) in enumerate(
            (
                (counts_hbm, counts_ref),
                (coords_hbm, coords_ref),
                (mass_hbm, mass_ref),
                (lists_hbm, list_v.at[R]),
                (lists_hbm.at[0], list_s.at[0]),
            )
        )
    ]
    for copy in inputs:
        copy.start()
    row_at = lax.broadcasted_iota(jnp.int32, (ROWS, 128), 0)
    lane_at = lax.broadcasted_iota(jnp.int32, (ROWS, 128), 1)
    slot_at = lax.rem(row_at, 2) * 128 + lane_at
    limit = jnp.zeros((ROWS, 128), jnp.int32)
    for copy in inputs:
        copy.wait()
    for t in range(TILES):
        limit = jnp.where(row_at // 2 == t, counts_ref[t], limit)
    filled = (slot_at < limit).astype(F32)
    own = slabs.at[R]
    own[pl.ds(0, ROWS, stride=4), :] = coords_ref[0:32, :] * (1.0 / R)
    own[pl.ds(1, ROWS, stride=4), :] = (coords_ref[32:64, :] - R) * (1.0 / R)
    own[pl.ds(2, ROWS, stride=4), :] = (coords_ref[64:96, :] - R) * (1.0 / R)
    own[pl.ds(3, ROWS, stride=4), :] = mass_ref[...] * filled
    list_row[...] = jnp.zeros_like(list_row)

    pl.semaphore_wait(barrier, 2 + has_low.astype(jnp.int32) + has_high.astype(jnp.int32))

    def wall_copy(slot, target):
        return pltpu.make_async_remote_copy(
            src_ref=own,
            dst_ref=walls.at[slot],
            send_sem=wall_send.at[slot],
            recv_sem=wall_recv.at[slot],
            device_id=(c, target),
            device_id_type=MESH,
        )

    def pass_on(source, k, target):
        slab = pltpu.make_async_remote_copy(
            src_ref=slabs.at[source],
            dst_ref=slabs.at[k - 1],
            send_sem=slab_send.at[k - 1],
            recv_sem=slab_recv.at[k - 1],
            device_id=target,
            device_id_type=MESH,
        )
        rows = pltpu.make_async_remote_copy(
            src_ref=list_v.at[source],
            dst_ref=list_v.at[k - 1],
            send_sem=list_send.at[k - 1],
            recv_sem=list_recv.at[k - 1],
            device_id=target,
            device_id_type=MESH,
        )
        return slab, rows

    def send(source, k, target):
        slab, rows = pass_on(source, k, target)
        rows.start()
        slab.start()

    def gain_copy(k):
        return pltpu.make_async_remote_copy(
            src_ref=gained.at[k],
            dst_ref=gained_in.at[k - 1],
            send_sem=gain_send.at[k - 1],
            recv_sem=gain_recv.at[k - 1],
            device_id=down(k),
            device_id_type=MESH,
        )

    def hand_copy(slot, target):
        return pltpu.make_async_remote_copy(
            src_ref=handed.at[pl.ds(64 * (1 - slot), ROWS)],
            dst_ref=handed_in.at[slot],
            send_sem=hand_send.at[slot],
            recv_sem=hand_recv.at[slot],
            device_id=(c, target),
            device_id_type=MESH,
        )

    crossing = c == chan_count - 2

    @pl.when(crossing)
    def _():
        send(R, 2, up(2))

    @pl.when(has_high)
    def _():
        wall_copy(0, w + 1).start()

    @pl.when(has_low)
    def _():
        wall_copy(1, w - 1).start()

    @pl.when(jnp.logical_not(crossing))
    def _():
        send(R, 2, up(2))

    @pl.when(first)
    def _():
        send(R, 1, partner)

    def list_down(k):
        return pltpu.make_async_copy(list_v.at[k - 1, k], list_s.at[k], list_copy.at[k])

    def build_b(packed, side):
        blocks = features_b(packed.reshape(TILES, 8, 128), 2.0 * (side - 1))
        tiles = slice(side * TILES, side * TILES + TILES)
        for half, (plain, triple, root, mass) in enumerate(blocks):
            lanes = slice(half * 128, half * 128 + 128)
            for at, rows in ((0, plain), (256, triple)):
                wide = slice(at + half * 128, at + half * 128 + 128)
                for g in range(0, 4, 2):
                    both = jnp.concatenate(rows[g : g + 2], axis=1).astype(BF16)
                    feat_b[tiles, 8 * g : 8 * g + 16, wide] = both
            root_b[tiles, 0:8, lanes] = root
            root_b[tiles, 8:16, lanes] = mass

    def build_a(feat, packed, shift):
        blocks = features_a(packed.reshape(TILES, 8, 128), shift)
        for half in range(2):
            for g in range(4):
                stage[half, :, 8 * g : 8 * g + 8, :] = blocks[half][g]
        for q in range(TILES // 4):
            for half in range(2):
                spot = q * TILE + half * 128
                turned = stage[half, 4 * q : 4 * q + 4].reshape(128, 128).T
                feat[spot : spot + 128, :] = turned.astype(BF16)

    build_a(feat_own, own[...], 0.0)
    build_b(own[...], 1)

    @pl.when(has_low)
    def _():
        wall_copy(0, w).wait_recv()

    @pl.when(jnp.logical_not(has_low))
    def _():
        walls[0] = jnp.zeros_like(walls[0])

    build_b(walls[0], 0)

    @pl.when(has_high)
    def _():
        wall_copy(1, w).wait_recv()

    @pl.when(jnp.logical_not(has_high))
    def _():
        walls[1] = jnp.zeros_like(walls[1])

    build_b(walls[1], 2)

    lane_row = lax.broadcasted_iota(jnp.int32, (1, 128), 1)
    pick_at = lax.broadcasted_iota(jnp.int32, (32, 128), 0)
    pick = jnp.logical_and(pick_at >= 27, pick_at < 30).astype(F32).astype(BF16)

    def placed(rows, quarter):
        width = rows.shape[1]
        parts = [jnp.zeros((32 * quarter, width), BF16)] if quarter else []
        parts.append(rows)
        if quarter < 3:
            parts.append(jnp.zeros((96 - 32 * quarter, width), BF16))
        return jnp.concatenate(parts, axis=0)


    def pair(dots, roots, mass, source, target):
        taken = jnp.zeros((8, TILE), F32)
        root = roots[0:8, :][None]
        top = roots[8:16, :][None]
        for r in range(0, TILE, CHUNK):
            square = dots[r : r + CHUNK, 0:TILE].reshape(CHUNK // 8, 8, TILE)
            triple = dots[r : r + CHUNK, TILE : 2 * TILE].reshape(CHUNK // 8, 8, TILE)
            near = root - square * lax.rsqrt(square)
            outer = near * near * near
            inner = top - triple * near
            value = lax.clamp(jnp.zeros_like(inner), outer, inner)
            low, high = value[:, :, 0:128], value[:, :, 128:256]
            row = (low + high).reshape(CHUNK, 128)
            if source is not None:
                row = row + source[r : r + CHUNK, :]
            target[r : r + CHUNK, :] = row
            weight = mass[r : r + CHUNK, :].reshape(CHUNK // 8, 8, 128)
            back = jnp.concatenate([low * weight, high * weight], axis=2)
            for e in range(CHUNK // 8):
                taken = taken + back[e]
        return jnp.sum(taken, axis=0, keepdims=True)

    def section(step, k, feat, begin, end):
        def a_tile(i):
            return feat[(i // 4) * TILE : (i // 4) * TILE + TILE, :]

        def dot_into(dots, i, n):
            rows = placed(feat_b[list_s[k, n, i]], i % 4)
            dots[...] = jnp.dot(a_tile(i), rows, preferred_element_type=F32)

        def mass_into(mass, i):
            mass[...] = jnp.dot(a_tile(i), placed(pick, i % 4), preferred_element_type=F32)

        def flush(i):
            summed = jnp.sum(full_g[...].T, axis=0, keepdims=True)
            gained[k, 2 * i : 2 * i + 1, :] = summed[:, 0:128]
            gained[k, 2 * i + 1 : 2 * i + 2, :] = summed[:, 128:256]

        def note(i, n, row):
            if step is not None:
                at = step * 32 + 2 * i + n
                handed_rows[pl.ds(at, 1), :] = row
                list_row[...] = jnp.where(lane_row == at, list_s[k, n, i], list_row[...])

        masses = (mass0, mass1)
        dot_into(dots0, begin, 0)
        mass_into(mass0, begin)
        for i in range(begin, end):
            mass = masses[(i - begin) % 2]
            dot_into(dots1, i, 1)
            if i > begin:
                flush(i - 1)
            note(i, 0, pair(dots0, root_b.at[list_s[k, 0, i]], mass, None, part_g))
            if i + 1 < end:
                dot_into(dots0, i + 1, 0)
                mass_into(masses[(i + 1 - begin) % 2], i + 1)
            note(i, 1, pair(dots1, root_b.at[list_s[k, 1, i]], mass, part_g, full_g))
        flush(end - 1)

    late = c < 2

    def take(k):
        slab, rows = pass_on(R, k, partner)
        rows.wait_recv()
        slab.wait_recv()

    def relay():
        take(2)
        send(1, 4, up(2))

        @pl.when(first)
        def _():
            send(1, 3, partner)

        @pl.when(jnp.logical_not(first))
        def _():
            send(1, 1, partner)

    pl.when(jnp.logical_not(late))(relay)
    section(None, 0, feat_own, 0, SPLIT)
    pl.when(jnp.logical_and(late, first))(relay)

    def one_offset(step, carry):
        near = jnp.where(first, 2 - step, 1 + step)
        k = jnp.where(step < 2, near, 6 - step)
        pl.when(jnp.logical_and(step == 1, jnp.logical_and(late, jnp.logical_not(first))))(relay)

        @pl.when(k != 2)
        def _():
            take(k)

        list_down(k).start()

        @pl.when(jnp.logical_and(step == 2, jnp.logical_not(first)))
        def _():
            send(3, 3, partner)

        build_a(feat_a, slabs[k - 1], k.astype(F32) * (1.0 / R))
        list_down(k).wait()
        section(step, k, feat_a, 0, TILES)
        gain_copy(k).start()
        return carry

    lax.fori_loop(0, R, one_offset, 0)

    known = list_row[...]
    hot = (lax.broadcasted_iota(jnp.int32, (48, 128), 0) == known).astype(F32).astype(BF16)
    summed = jnp.zeros((48, TILE), F32)
    for piece in split3(handed_rows[...]):
        summed = summed + jnp.dot(hot, piece.astype(BF16), preferred_element_type=F32)
    handed[pl.ds(0, 48, stride=2), :] = summed[:, 0:128]
    handed[pl.ds(1, 48, stride=2), :] = summed[:, 128:256]

    @pl.when(has_high)
    def _():
        hand_copy(0, w + 1).start()

    @pl.when(has_low)
    def _():
        hand_copy(1, w - 1).start()

    section(None, 0, feat_own, SPLIT, TILES)

    total = gained[0]
    for k in range(1, R + 1):
        gain_copy(k).wait_recv()
        total = total + gained_in[k - 1]
    out_ref[...] = handed[32:64, :]

    @pl.when(has_low)
    def _():
        hand_copy(0, w).wait_recv()
        out_ref[...] += handed_in[0]

    @pl.when(has_high)
    def _():
        hand_copy(1, w).wait_recv()
        out_ref[...] += handed_in[1]

    scale = filled * (1.0 / (4.0 * math.pi * 2 * TILE))
    out_ref[...] = (total + out_ref[...] / mass_ref[...]) * scale

    for k in range(1, R + 1):
        slab, rows = pass_on(R, k, partner)
        slab.wait_send()
        rows.wait_send()
        gain_copy(k).wait_send()

    @pl.when(has_high)
    def _():
        wall_copy(0, w).wait_send()
        hand_copy(0, w).wait_send()

    @pl.when(has_low)
    def _():
        wall_copy(1, w).wait_send()
        hand_copy(1, w).wait_send()


def solution(mesh):
    placed = (
        P(None, "chan", "wall", None),
        P("chan", "wall", None),
        P("chan", "wall", None),
        P("chan", "wall", None, None, None),
    )
    chan_count = mesh.shape["chan"]
    wall_count = mesh.shape["wall"]

    def on_device(coords, masses, counts, lists):
        vmem = pl.BlockSpec(memory_space=pltpu.VMEM)
        hbm = pl.BlockSpec(memory_space=pl.ANY)
        dma = pltpu.SemaphoreType.DMA
        density = pl.pallas_call(
            functools.partial(kernel, chan_count, wall_count),
            out_shape=pltpu.VMEM((ROWS, 128), F32),
            in_specs=[hbm, hbm, hbm, hbm],
            out_specs=vmem,
            scratch_shapes=[
                pltpu.VMEM((3 * ROWS, 128), F32),
                pltpu.VMEM((ROWS, 128), F32),
                pltpu.SMEM((TILES,), jnp.int32),
                dma((5,)),
                pltpu.VMEM((2, 128, 128), F32),
                pltpu.VMEM((R + 1, 128, 128), F32),
                pltpu.VMEM((R + 1, R + 1, 2, 16), jnp.int32),
                pltpu.SMEM((R + 1, 2, 16), jnp.int32),
                pltpu.VMEM((2, TILES, 32, 128), F32),
                pltpu.VMEM((48, 32, 512), BF16),
                pltpu.VMEM((48, 16, TILE), F32),
                pltpu.VMEM((4 * TILE, 128), BF16),
                pltpu.VMEM((4 * TILE, 128), BF16),
                pltpu.VMEM((TILE, 512), F32),
                pltpu.VMEM((TILE, 512), F32),
                pltpu.VMEM((TILE, 128), F32),
                pltpu.VMEM((TILE, 128), F32),
                pltpu.VMEM((TILE, 128), F32),
                pltpu.VMEM((TILE, 128), F32),
                pltpu.VMEM((R + 1, ROWS, 128), F32),
                pltpu.VMEM((R, ROWS, 128), F32),
                pltpu.VMEM((32 * R, TILE), F32),
                pltpu.VMEM((1, 128), jnp.int32),
                pltpu.VMEM((96, 128), F32),
                pltpu.VMEM((2, ROWS, 128), F32),
                dma((R,)),
                dma((R,)),
                dma((2,)),
                dma((2,)),
                dma((R,)),
                dma((R,)),
                dma((R,)),
                dma((R,)),
                dma((2,)),
                dma((2,)),
                dma((R + 1,)),
            ],
            compiler_params=pltpu.CompilerParams(
                collective_id=0,
                has_side_effects=True,
            ),
        )(
            coords.reshape(3 * ROWS, 128),
            masses.reshape(ROWS, 128),
            counts.reshape(TILES),
            jnp.transpose(lists.reshape(R + 1, TILES, 2), (0, 2, 1)),
        )
        return density.reshape(1, 1, -1)

    return jax.shard_map(
        on_device, mesh=mesh, in_specs=placed, out_specs=P("chan", "wall", None), check_vma=False
    )
```
